32 devices in a mesh: half: 2 (over core), blk: 4 (over z), sub: 4 (over y, x).
Axes of the slice: x: 2, y: 2, z: 4, core: 2. Of those that a mesh axis runs over, the one named last changes fastest.
Arguments:
- leaf_expansions: float32 [16384, 128], P(('half', 'blk', 'sub')), may hold values from -0.3 to 0.3
- leaf_occupied: int32 [16384], P(('half', 'blk', 'sub')), may hold values 0 or 1
- cone_angles: float32 [2, 48], replicated, may hold values from -3.140625 to 3.140625
- cone_need3: int32 [48, 32], P(('half', 'blk'), 'sub'), may hold values 0 or 1
- cone_need4: int32 [48, 4], P(('half', 'blk'), 'sub'), may hold values 0 or 1
Outputs:
- lowfreq: float32 [256, 128], P(('half', 'blk', 'sub'))
- cone_expansions: float32 [48, 4, 128], P(('half', 'blk'), 'sub')
The draws below stay inside these ranges and needn't reach their ends.
All inputs are finite; a program needn't handle non-finite values. No bound on the sum of `leaf_occupied` or of `cone_need3` or of `cone_need4` on one device may be relied on, other than what follows from the above.
Results may differ from the reference program's by a relative error of at most 0.00007.
Values sent between devices are 32-bit elements; how exact they have to be, the bound alone decides.
A program may use at most 64 MiB of HBM per device.

```python
import math
import jax
import jax.numpy as jnp
from jax import lax

ORDER = 4
NODES = 64
CONE_DEV = 6
CONES = 48
LEAF_DEV = 512
LEAVES = 16384
BOX3 = 32
BOX4 = 4
N_HALF = 2
N_BLK = 4
N_SUB = 4


def touch_ends(values, stream_key, smallest, top_value):
    spot = [jax.random.randint(jax.random.fold_in(stream_key, axis), (), 0, length) for axis, length in enumerate(values.shape)]
    longest = values.shape.index(max(values.shape))
    neighbour = spot[:longest] + [(spot[longest] + 1) % values.shape[longest]] + spot[longest + 1:]
    return values.at[tuple(spot)].set(smallest).at[tuple(neighbour)].set(top_value)


def shard_levels(own_key, dims, shards, low, high):
    loudness, own = 1.0, jax.random.fold_in(own_key, 6)
    for dim, parts in shards:
        heights = jnp.exp(jax.random.uniform(jax.random.fold_in(own, dim), (parts,), jnp.float32, low / len(shards), high / len(shards)))
        loudness = loudness * jnp.repeat(heights, dims[dim] // parts).reshape([-1 if axis == dim else 1 for axis in range(len(dims))])
    return loudness


def scatter_about(rng, dims, deviation, most, shards=(), kind=jnp.bfloat16):
    values = deviation * jax.random.normal(rng, dims, jnp.float32)
    if shards:
        values = values * shard_levels(rng, dims, shards, -0.22, 0.18)
    return jnp.clip(values, -most, most).astype(kind)


def setup_inputs(seed: int = 0) -> dict:
    arg_keys = jax.random.split(jax.random.key(seed), 6)
    return {
        "leaf_expansions": scatter_about(arg_keys[0], (LEAVES, 2 * NODES), 0.05, 0.3, ((0, 32),), jnp.float32),
        "leaf_occupied": touch_ends((jax.random.randint(arg_keys[1], (LEAVES,), 0, 2) < 1).astype(jnp.int32), jax.random.fold_in(arg_keys[1], 1), 0, 1),
        "cone_angles": jnp.clip(jax.random.uniform(arg_keys[2], (2, CONES), jnp.float32, -3.140625, 3.140625), -3.140625, 3.140625),
        "cone_need3": touch_ends((jax.random.randint(arg_keys[3], (CONES, BOX3), 0, 4) < 3).astype(jnp.int32), jax.random.fold_in(arg_keys[3], 1), 0, 1),
        "cone_need4": touch_ends((jax.random.randint(arg_keys[4], (CONES, BOX4), 0, 4) < 3).astype(jnp.int32), jax.random.fold_in(arg_keys[4], 1), 0, 1),
    }


near_scale = 1.5
far_scale = 3.0
highest = lax.Precision.HIGHEST


def chebyshev_points(per_axis):
    index = jnp.arange(per_axis, dtype=jnp.float32)
    return jnp.cos((2.0 * index + 1.0) * math.pi / (2.0 * per_axis))


def octant_signs():
    octant = jnp.arange(8, dtype=jnp.int32)
    bits = jnp.stack([(octant // 4) % 2, (octant // 2) % 2, octant % 2], -1)
    return bits.astype(jnp.float32) * 2.0 - 1.0


def octant_table(per_axis):
    points = chebyshev_points(per_axis)
    degree = jnp.arange(1, per_axis, dtype=jnp.float32)
    sign_pair = jnp.array([-1.0, 1.0], dtype=jnp.float32)
    shifted = (points[None, :] + sign_pair[:, None]) / 2.0
    poly_here = jnp.cos(degree[None, :] * jnp.arccos(points)[:, None])
    poly_there = jnp.cos(degree[None, None, :] * jnp.arccos(shifted)[:, :, None])
    single = 1.0 / per_axis + (2.0 / per_axis) * jnp.einsum('mk,bnk->bmn', poly_here, poly_there, precision=highest)
    signs = octant_signs()
    along_x = jnp.where((signs[:, 0] > 0)[:, None, None], single[1][None], single[0][None])
    along_y = jnp.where((signs[:, 1] > 0)[:, None, None], single[1][None], single[0][None])
    along_z = jnp.where((signs[:, 2] > 0)[:, None, None], single[1][None], single[0][None])
    full = jnp.einsum('oad,obe,ocf->odefabc', along_x, along_y, along_z, precision=highest)
    node_count = per_axis ** 3
    return full.reshape(8, node_count, node_count)


def node_offsets(per_axis):
    points = chebyshev_points(per_axis)
    index = jnp.arange(per_axis ** 3, dtype=jnp.int32)
    coords = jnp.stack([points[index // (per_axis * per_axis)], points[(index // per_axis) % per_axis], points[index % per_axis]], -1)
    return coords[None, :, :] + octant_signs()[:, None, :]


def phases(angles, strength, per_axis):
    polar = angles[0]
    azimuth = angles[1]
    direction = jnp.stack([jnp.sin(polar) * jnp.cos(azimuth), jnp.sin(polar) * jnp.sin(azimuth), jnp.cos(polar)], -1)
    offsets = node_offsets(per_axis)
    argument = offsets[None, :, :, 0] * direction[:, None, None, 0]
    argument = argument + offsets[None, :, :, 1] * direction[:, None, None, 1]
    argument = argument + offsets[None, :, :, 2] * direction[:, None, None, 2]
    argument = -strength * argument
    return jnp.cos(argument), jnp.sin(argument)


def interpolate(real_part, imag_part, cosines, sine_part, transfer):
    mod_real = cosines * real_part - sine_part * imag_part
    mod_imag = cosines * imag_part + sine_part * real_part
    out_real = jnp.einsum('...on,onm->...m', mod_real, transfer, precision=highest)
    out_imag = jnp.einsum('...on,onm->...m', mod_imag, transfer, precision=highest)
    return out_real, out_imag


def reference(leaf_expansions, leaf_occupied, cone_angles, cone_need3, cone_need4):
    node_count = NODES
    groups = N_HALF * N_BLK
    level_one_count = LEAF_DEV // 8
    pair_count = level_one_count // 2
    per_sub = pair_count // N_SUB
    per_box = per_sub // 8
    transfer = octant_table(ORDER)
    masked = leaf_expansions * leaf_occupied.astype(jnp.float32)[:, None]
    masked = masked.reshape(groups, N_SUB, level_one_count, 8, 2, node_count)
    level_one = jnp.einsum('gspoan,onm->gspam', masked, transfer, precision=highest)
    level_one = level_one.reshape(groups, N_SUB, pair_count, 2, 2, node_count)
    level_one = jnp.transpose(level_one, (0, 2, 1, 3, 4, 5)).reshape(groups, pair_count, 2 * N_SUB, 2, node_count)
    level_two = jnp.einsum('gkoan,onm->gkam', level_one, transfer[:2 * N_SUB], precision=highest)
    lowfreq = level_two.reshape(groups * pair_count, 2 * node_count)
    box_rows = level_two.reshape(groups, N_SUB, per_box, 8, 2, node_count)
    box_rows = jnp.transpose(box_rows, (1, 0, 2, 3, 4, 5)).reshape(N_SUB * groups * per_box, 8, 2, node_count)
    real_part = box_rows[:, :, 0, :]
    imag_part = box_rows[:, :, 1, :]
    angle_blocks = jnp.transpose(cone_angles.reshape(2, groups, CONE_DEV), (1, 0, 2))
    need_three = cone_need3.reshape(groups, CONE_DEV, -1)
    need_four = cone_need4.reshape(groups, CONE_DEV, -1)

    def one_block(inputs):
        angles, mask_three, mask_four = inputs
        cos_near, sin_near = phases(angles, near_scale, ORDER)
        three_real, three_imag = interpolate(real_part[None], imag_part[None], cos_near[:, None], sin_near[:, None], transfer)
        weight = mask_three.astype(jnp.float32)[:, :, None]
        three_real = three_real * weight
        three_imag = three_imag * weight
        shape_six = (CONE_DEV, N_SUB, groups // 8, 8, per_box, node_count)
        three_real = jnp.transpose(three_real.reshape(shape_six), (0, 1, 2, 4, 3, 5)).reshape(CONE_DEV, -1, 8, node_count)
        three_imag = jnp.transpose(three_imag.reshape(shape_six), (0, 1, 2, 4, 3, 5)).reshape(CONE_DEV, -1, 8, node_count)
        cos_far, sin_far = phases(angles, far_scale, ORDER)
        four_real, four_imag = interpolate(three_real, three_imag, cos_far[:, None], sin_far[:, None], transfer)
        joined = jnp.concatenate([four_real, four_imag], -1)
        return joined * mask_four.astype(jnp.float32)[:, :, None]

    cone_expansions = lax.map(one_block, (angle_blocks, need_three, need_four))
    cone_expansions = cone_expansions.reshape(CONES, -1, 2 * node_count)
    return lowfreq, cone_expansions
```

```python
import functools
import math

import jax
import jax.numpy as jnp
import numpy as np
from jax import lax
from jax.experimental import pallas as pl
from jax.experimental.pallas import tpu as pltpu
from jax.sharding import PartitionSpec as P

MESH = pl.DeviceIdType.MESH
F32, BF16 = jnp.float32, jnp.bfloat16
ORDER = 4
OCT = 8
NEAR = 1.5


def octant_signs():
    octant = np.arange(OCT)
    return np.stack([octant // 4 % 2, octant // 2 % 2, octant % 2], -1) * 2.0 - 1.0


def chebyshev_points(per_axis):
    return np.cos((2.0 * np.arange(per_axis) + 1.0) * math.pi / (2.0 * per_axis))


def octant_table(per_axis):
    points = chebyshev_points(per_axis)
    degree = np.arange(1, per_axis)
    shifted = (points[None, :] + np.array([-1.0, 1.0])[:, None]) / 2.0
    here = np.cos(degree[None, :] * np.arccos(points)[:, None])
    there = np.cos(degree * np.arccos(shifted)[:, :, None])
    single = 1.0 / per_axis + 2.0 / per_axis * np.einsum("mk,bnk->bnm", here, there)
    bit = (octant_signs() > 0).astype(int)
    full = np.einsum("oda,oeb,ofc->odefabc", single[bit[:, 0]], single[bit[:, 1]], single[bit[:, 2]])
    return full.reshape(OCT, per_axis**3, per_axis**3)


def weight_table(per_axis):
    table = octant_table(per_axis).astype(np.float32)
    nodes = per_axis**3
    wide = np.zeros((OCT, 2, nodes, 2, nodes), np.float32)
    wide[:, 0, :, 0, :] = table
    wide[:, 1, :, 1, :] = table
    wide = wide.reshape(OCT * 2 * nodes, 2 * nodes)
    high = wide.astype(BF16)
    low = (wide - high.astype(np.float32)).astype(BF16)
    return np.concatenate([high, low], 1)


def lane_table(per_axis):
    points = chebyshev_points(per_axis)
    index = np.arange(per_axis**3)
    coords = np.stack([points[index // per_axis**2], points[index // per_axis % per_axis], points[index % per_axis]])
    offsets = coords[:, None, :] + octant_signs().T[:, :, None]
    offsets = -NEAR * np.concatenate([offsets, offsets], -1).reshape(3, -1)
    sign = np.tile(np.repeat([-1.0, 1.0], per_axis**3), OCT)
    return np.concatenate([offsets, sign[None]], 0).astype(np.float32)


def each(start, count, body):
    if count - start <= 64:
        for d in range(start, count):
            body(d)
    else:
        lax.fori_loop(start, count, lambda d, c: (body(d), c)[1], 0)


def split_rows(value):
    high = value.astype(BF16)
    low = (value - high.astype(F32)).astype(BF16)
    return jnp.concatenate([high, low], 0)


def fold(acc, rows, width):
    return (acc[:rows, :width] + acc[rows:, :width]) + (acc[:rows, width:] + acc[rows:, width:])


def kernel(
    halves, blks, subs, cones,
    leaf_hbm, occ_hbm, angle_hbm, need3_hbm, need4_hbm, weight_hbm, lane_hbm,
    low_out, cone_out,
    leaf, occ, angle, need3, need4, weight, lane, part, got, mine, theirs, three, phase,
    in_sem, send, recv, send2, recv2,
):
    groups = halves * blks
    half, blk, sub = lax.axis_index("half"), lax.axis_index("blk"), lax.axis_index("sub")
    group = half * blks + blk
    rows, width = leaf.shape
    pairs = rows // (2 * OCT)
    per_sub = pairs // subs

    loads = [
        pltpu.make_async_copy(src, dst, in_sem.at[i])
        for i, (src, dst) in enumerate([
            (occ_hbm, occ), (leaf_hbm, leaf), (weight_hbm, weight), (angle_hbm, angle),
            (lane_hbm, lane), (need3_hbm, need3), (need4_hbm, need4),
        ])
    ]
    for load in loads:
        load.start()

    other = halves - 1 - half

    def blk_of(j):
        return lax.rem(j + blks - 1 - blk, blks)

    def sub_of(t):
        return lax.rem(t + subs - 1 - sub, subs)

    def peer(d):
        return {"half": other, "blk": blk_of(d // subs), "sub": sub_of(lax.rem(d, subs))}

    barrier = pltpu.get_barrier_semaphore()
    each(
        0, blks * subs,
        lambda d: pl.semaphore_signal(barrier, inc=1, device_id=peer(d), device_id_type=MESH),
    )

    loads[0].wait()
    loads[1].wait()
    columns = jnp.transpose(occ[...].astype(F32))
    for i in range(rows // 128):
        chunk = pl.ds(i * 128, 128)
        leaf[chunk, :] = leaf[chunk, :] * columns[:, i : i + 1]
    loads[2].wait()
    acc = None
    for t in range(OCT // 2):
        tile = jnp.concatenate(
            [
                jnp.concatenate(
                    [leaf[pl.ds(OCT * r + o, pairs, stride=2 * OCT), :] for o in (2 * t, 2 * t + 1)], 1
                )
                for r in range(2)
            ],
            0,
        )
        term = jnp.dot(
            split_rows(tile), weight[2 * width * t : 2 * width * (t + 1), :], preferred_element_type=F32
        )
        acc = term if acc is None else acc + term
    one = fold(acc, 2 * pairs, width)
    tile = jnp.concatenate([one[:pairs], one[pairs:]], 1)
    ours = weight[pl.ds(pl.multiple_of(sub * 2 * width, 2 * width), 2 * width), :]
    part[...] = fold(jnp.dot(split_rows(tile), ours, preferred_element_type=F32), pairs, width)

    pl.semaphore_wait(barrier, blks * subs)

    def copy(d):
        there = peer(d)
        return pltpu.make_async_remote_copy(
            src_ref=part.at[pl.ds(pl.multiple_of(there["sub"] * per_sub, 8), per_sub)],
            dst_ref=got.at[d // subs * subs + sub],
            send_sem=send.at[0],
            recv_sem=recv.at[jnp.minimum(d // subs, 1)],
            device_id=there,
            device_id_type=MESH,
        )

    each(0, blks * subs, lambda d: copy(d).start())

    loads[3].wait()
    loads[4].wait()
    padded = phase.shape[1]
    count = angle.shape[1]
    pick = lax.broadcasted_iota(jnp.int32, (padded, count), 1) == (
        lax.broadcasted_iota(jnp.int32, (padded, count), 0) + group * cones
    )
    polar = jnp.sum(jnp.where(pick, angle[0:1, :], 0.0), 1, keepdims=True)
    azimuth = jnp.sum(jnp.where(pick, angle[1:2, :], 0.0), 1, keepdims=True)
    sin_polar = jnp.sin(polar)
    argument = (
        (sin_polar * jnp.cos(azimuth)) * lane[0:1, :]
        + (sin_polar * jnp.sin(azimuth)) * lane[1:2, :]
        + jnp.cos(polar) * lane[2:3, :]
    )
    cosine, sine = jnp.cos(argument), jnp.sin(argument)
    sign = lane[3:4, :]
    phase[0] = cosine
    phase[1] = sine * sign
    phase[2] = 1.0 - 2.0 * sine * sine
    phase[3] = 2.0 * sine * cosine * sign
    loads[5].wait()
    loads[6].wait()

    def widen(value):
        fill = padded - cones
        if fill:
            value = jnp.concatenate([value, jnp.zeros((fill, value.shape[1]), value.dtype)], 0)
        return value.astype(F32)

    keep3 = widen(need3[...])
    lanes4 = need4.shape[1]
    diagonal = lax.broadcasted_iota(jnp.int32, (padded, lanes4), 0) == lax.broadcasted_iota(
        jnp.int32, (padded, lanes4), 1
    )

    def product(pieces):
        rows_in = pieces[0].shape[0]
        acc = None
        for t in range(OCT // 2):
            tile = split_rows(jnp.concatenate(pieces[2 * t : 2 * t + 2], 1))
            term = jnp.dot(tile, weight[2 * width * t : 2 * width * (t + 1), :], preferred_element_type=F32)
            acc = term if acc is None else acc + term
        return fold(acc, rows_in, width)

    def level_three(start, size):
        named = [
            (box, first + blk_of(j))
            for j in range(start, start + size)
            for box, first in ((mine[j], other * blks), (theirs[j], half * blks))
        ]
        boxes = [box for box, _ in named]
        turned = [pltpu.roll(box, width // 2, 1) for box in boxes]
        pieces = []
        for o in range(OCT):
            lanes = slice(o * width, (o + 1) * width)
            cos_o, sin_o = phase[0, :, lanes], phase[1, :, lanes]
            pieces.append(
                jnp.concatenate(
                    [cos_o * box[o : o + 1, :] + sin_o * turn[o : o + 1, :] for box, turn in zip(boxes, turned)], 0
                )
            )
        result = product(pieces)
        for g, (_, index) in enumerate(named):
            three[index] = result[g * padded : (g + 1) * padded]

    far, near = pl.ds(0, 1), pl.ds(1, blks - 1)

    def landed(k):
        slots = got.at[pl.ds(0, subs)] if k == 0 else got.at[pl.ds(subs, (blks - 1) * subs)]
        return pltpu.make_async_copy(slots, slots, recv.at[k])

    def total(j):
        mine[j] = functools.reduce(jnp.add, [got[j * subs + t] for t in range(subs)])

    def forward(k):
        boxes = far if k == 0 else near
        return pltpu.make_async_remote_copy(
            src_ref=mine.at[boxes],
            dst_ref=theirs.at[boxes],
            send_sem=send2.at[0],
            recv_sem=recv2.at[k],
            device_id={"half": other},
            device_id_type=MESH,
        )

    landed(1).wait()
    each(1, blks, total)
    forward(1).start()
    landed(0).wait()
    total(0)
    forward(0).start()
    forward(1).wait_recv()
    for start in range(1, blks, 3):
        level_three(start, min(3, blks - start))
    forward(0).wait_recv()
    low_out[...] = theirs[lax.rem(2 * blk + 1, blks)]
    level_three(0, 1)

    for q in range(groups // OCT):
        pieces = []
        for o in range(OCT):
            lanes = slice(o * width, (o + 1) * width)
            column = q * OCT + o
            box = three[column] * keep3[:, column : column + 1]
            pieces.append(phase[2, :, lanes] * box + phase[3, :, lanes] * pltpu.roll(box, width // 2, 1))
        keep4 = jnp.sum(jnp.where(diagonal, need4[q : q + 1, :].astype(F32), 0.0), 1, keepdims=True)
        four = product(pieces) * keep4
        cone_out[:, q, :] = four[:cones]

    pltpu.make_async_copy(got, got, send.at[0]).wait()
    pltpu.make_async_copy(mine, mine, send2.at[0]).wait()


def put_out(low_ref, cone_ref, low_out, cone_out, sems):
    copies = [
        pltpu.make_async_copy(low_ref, low_out, sems.at[0]),
        pltpu.make_async_copy(cone_ref, cone_out, sems.at[1]),
    ]
    for copy in copies:
        copy.start()
    for copy in copies:
        copy.wait()


def solution(mesh):
    halves, blks, subs = mesh.shape["half"], mesh.shape["blk"], mesh.shape["sub"]
    groups = halves * blks

    def local(leaf, occupied, angles, need3, need4):
        rows, width = leaf.shape
        pairs = rows // (2 * OCT)
        per_sub = pairs // subs
        cones = need3.shape[0]
        padded = -(-cones // 8) * 8
        assert per_sub == OCT and need3.shape[1] == groups and halves == 2
        weight = jnp.asarray(weight_table(ORDER))
        lane = jnp.asarray(lane_table(ORDER))
        occupied = occupied.reshape(rows // 128, 128)
        need4 = need4.T
        vmem = pl.BlockSpec(memory_space=pltpu.VMEM)
        anywhere = pl.BlockSpec(memory_space=pl.ANY)
        results = pl.pallas_call(
            functools.partial(kernel, halves, blks, subs, cones),
            out_shape=(
                pltpu.VMEM((per_sub, width), F32),
                pltpu.VMEM((cones, groups // OCT, width), F32),
            ),
            in_specs=[anywhere] * 7,
            out_specs=(vmem, vmem),
            scratch_shapes=[
                pltpu.VMEM(leaf.shape, F32),
                pltpu.VMEM(occupied.shape, jnp.int32),
                pltpu.VMEM(angles.shape, F32),
                pltpu.VMEM(need3.shape, jnp.int32),
                pltpu.VMEM(need4.shape, jnp.int32),
                pltpu.VMEM(weight.shape, BF16),
                pltpu.VMEM(lane.shape, F32),
                pltpu.VMEM((pairs, width), F32),
                pltpu.VMEM((blks * subs, per_sub, width), F32),
                pltpu.VMEM((blks, per_sub, width), F32),
                pltpu.VMEM((blks, per_sub, width), F32),
                pltpu.VMEM((groups, padded, width), F32),
                pltpu.VMEM((4, padded, OCT * width), F32),
                pltpu.SemaphoreType.DMA((7,)),
                pltpu.SemaphoreType.DMA((1,)),
                pltpu.SemaphoreType.DMA((2,)),
                pltpu.SemaphoreType.DMA((1,)),
                pltpu.SemaphoreType.DMA((2,)),
            ],
            compiler_params=pltpu.CompilerParams(collective_id=0, has_side_effects=True),
            name="upward",
        )(leaf, occupied, angles, need3, need4, weight, lane)
        results = [pltpu.with_memory_space_constraint(value, pltpu.VMEM) for value in results]
        return pl.pallas_call(
            put_out,
            out_shape=[jax.ShapeDtypeStruct(value.shape, F32) for value in results],
            in_specs=[vmem] * 2,
            out_specs=[pl.BlockSpec(memory_space=pltpu.HBM)] * 2,
            scratch_shapes=[pltpu.SemaphoreType.DMA((2,))],
            name="put_out",
        )(*results)

    return jax.shard_map(
        local,
        mesh=mesh,
        in_specs=(
            P(("half", "blk", "sub"), None),
            P(("half", "blk", "sub")),
            P(),
            P(("half", "blk"), "sub"),
            P(("half", "blk"), "sub"),
        ),
        out_specs=(P(("half", "blk", "sub"), None), P(("half", "blk"), "sub", None)),
        check_vma=False,
    )
```

```python
import functools
import math
import operator

import jax
import jax.numpy as jnp
import numpy as np
from jax import lax
from jax.experimental import pallas as pl
from jax.experimental.pallas import tpu as pltpu
from jax.sharding import PartitionSpec as P

MESH = pl.DeviceIdType.MESH
F32, BF16 = jnp.float32, jnp.bfloat16
ORDER = 4
OCT = 8
NEAR = 1.5


def octant_signs():
    octant = np.arange(OCT)
    return np.stack([octant // 4 % 2, octant // 2 % 2, octant % 2], -1) * 2.0 - 1.0


def chebyshev_points(per_axis):
    return np.cos((2.0 * np.arange(per_axis) + 1.0) * math.pi / (2.0 * per_axis))


def octant_table(per_axis):
    points = chebyshev_points(per_axis)
    degree = np.arange(1, per_axis)
    shifted = (points[None, :] + np.array([-1.0, 1.0])[:, None]) / 2.0
    here = np.cos(degree[None, :] * np.arccos(points)[:, None])
    there = np.cos(degree * np.arccos(shifted)[:, :, None])
    single = 1.0 / per_axis + 2.0 / per_axis * np.einsum("mk,bnk->bnm", here, there)
    bit = (octant_signs() > 0).astype(int)
    full = np.einsum("oda,oeb,ofc->odefabc", single[bit[:, 0]], single[bit[:, 1]], single[bit[:, 2]])
    return full.reshape(OCT, per_axis**3, per_axis**3)


def weight_table(per_axis):
    table = octant_table(per_axis).astype(np.float32)
    nodes = per_axis**3
    wide = np.zeros((OCT, 2, nodes, 2, nodes), np.float32)
    wide[:, 0, :, 0, :] = table
    wide[:, 1, :, 1, :] = table
    wide = wide.reshape(OCT * 2 * nodes, 2 * nodes)
    high = wide.astype(BF16)
    low = (wide - high.astype(np.float32)).astype(BF16)
    return np.concatenate([high, low], 1)


def lane_table(per_axis):
    points = chebyshev_points(per_axis)
    index = np.arange(per_axis**3)
    coords = np.stack([points[index // per_axis**2], points[index // per_axis % per_axis], points[index % per_axis]])
    offsets = coords[:, None, :] + octant_signs().T[:, :, None]
    offsets = -NEAR * np.concatenate([offsets, offsets], -1).reshape(3, -1)
    sign = np.tile(np.repeat([-1.0, 1.0], per_axis**3), OCT)
    return np.concatenate([offsets, sign[None]], 0).astype(np.float32)


def each(start, count, body):
    if count - start <= 64:
        for d in range(start, count):
            body(d)
    else:
        lax.fori_loop(start, count, lambda d, c: (body(d), c)[1], 0)


def split_rows(value):
    high = value.astype(BF16)
    low = (value - high.astype(F32)).astype(BF16)
    return jnp.concatenate([high, low], 0)


def fold(acc, rows, width):
    return (acc[:rows, :width] + acc[rows:, :width]) + (acc[:rows, width:] + acc[rows:, width:])


def kernel(
    halves, blks, subs, cones,
    leaf_hbm, occ_hbm, angle_hbm, need3_hbm, need4_hbm, weight_hbm, lane_hbm,
    low_out, cone_out,
    leaf, occ, angle, need3, need4, weight, lane, part, got, mine, theirs, three, phase,
    in_sem, send, recv, send2, recv2, ready,
):
    groups = halves * blks
    half, blk, sub = lax.axis_index("half"), lax.axis_index("blk"), lax.axis_index("sub")
    group = half * blks + blk
    rows, width = leaf.shape
    pairs = rows // (2 * OCT)
    per_sub = pairs // subs

    loads = [
        pltpu.make_async_copy(src, dst, in_sem.at[i])
        for i, (src, dst) in enumerate([
            (occ_hbm, occ), (leaf_hbm, leaf), (weight_hbm, weight), (angle_hbm, angle),
            (lane_hbm, lane), (need3_hbm, need3), (need4_hbm, need4),
        ])
    ]
    for load in loads:
        load.start()

    other = halves - 1 - half

    def blk_of(j):
        return lax.rem(j + blks - 1 - blk, blks)

    def sub_of(t):
        return lax.rem(t + subs - 1 - sub, subs)

    def peer(d):
        return {"half": other, "blk": blk_of(d // subs), "sub": sub_of(lax.rem(d, subs))}

    def planes(wanted, act):
        def plane(j):
            @pl.when(wanted(blk_of(j), blk))
            def _():
                each(0, subs, lambda t: act(j * subs + t))

        each(0, blks, plane)

    def greet(semaphore):
        return lambda d: pl.semaphore_signal(semaphore, inc=1, device_id=peer(d), device_id_type=MESH)

    barrier = pltpu.get_barrier_semaphore()
    planes(operator.ge, greet(barrier))

    loads[0].wait()
    loads[1].wait()
    columns = jnp.transpose(occ[...].astype(F32))
    for i in range(rows // 128):
        chunk = pl.ds(i * 128, 128)
        leaf[chunk, :] = leaf[chunk, :] * columns[:, i : i + 1]
    loads[2].wait()
    acc = None
    for t in range(OCT // 2):
        tile = jnp.concatenate(
            [
                jnp.concatenate(
                    [leaf[pl.ds(OCT * r + o, pairs, stride=2 * OCT), :] for o in (2 * t, 2 * t + 1)], 1
                )
                for r in range(2)
            ],
            0,
        )
        term = jnp.dot(
            split_rows(tile), weight[2 * width * t : 2 * width * (t + 1), :], preferred_element_type=F32
        )
        acc = term if acc is None else acc + term
    one = fold(acc, 2 * pairs, width)
    tile = jnp.concatenate([one[:pairs], one[pairs:]], 1)
    ours = weight[pl.ds(pl.multiple_of(sub * 2 * width, 2 * width), 2 * width), :]
    part[...] = fold(jnp.dot(split_rows(tile), ours, preferred_element_type=F32), pairs, width)

    pl.semaphore_wait(barrier, (blk + 1) * subs)

    def copy(d):
        there = peer(d)
        return pltpu.make_async_remote_copy(
            src_ref=part.at[pl.ds(pl.multiple_of(there["sub"] * per_sub, 8), per_sub)],
            dst_ref=got.at[d // subs * subs + sub],
            send_sem=send.at[0],
            recv_sem=recv.at[jnp.minimum(d // subs, 1)],
            device_id=there,
            device_id_type=MESH,
        )

    planes(operator.le, lambda d: copy(d).start())
    planes(operator.lt, lambda d: greet(ready.at[d // subs])(d))

    loads[3].wait()
    loads[4].wait()
    padded = phase.shape[1]
    count = angle.shape[1]
    pick = lax.broadcasted_iota(jnp.int32, (padded, count), 1) == (
        lax.broadcasted_iota(jnp.int32, (padded, count), 0) + group * cones
    )
    polar = jnp.sum(jnp.where(pick, angle[0:1, :], 0.0), 1, keepdims=True)
    azimuth = jnp.sum(jnp.where(pick, angle[1:2, :], 0.0), 1, keepdims=True)
    sin_polar = jnp.sin(polar)
    argument = (
        (sin_polar * jnp.cos(azimuth)) * lane[0:1, :]
        + (sin_polar * jnp.sin(azimuth)) * lane[1:2, :]
        + jnp.cos(polar) * lane[2:3, :]
    )
    cosine, sine = jnp.cos(argument), jnp.sin(argument)
    sign = lane[3:4, :]
    phase[0] = cosine
    phase[1] = sine * sign
    phase[2] = 1.0 - 2.0 * sine * sine
    phase[3] = 2.0 * sine * cosine * sign
    loads[5].wait()
    loads[6].wait()

    def widen(value):
        fill = padded - cones
        if fill:
            value = jnp.concatenate([value, jnp.zeros((fill, value.shape[1]), value.dtype)], 0)
        return value.astype(F32)

    keep3 = widen(need3[...])
    lanes4 = need4.shape[1]
    diagonal = lax.broadcasted_iota(jnp.int32, (padded, lanes4), 0) == lax.broadcasted_iota(
        jnp.int32, (padded, lanes4), 1
    )

    def product(pieces):
        rows_in = pieces[0].shape[0]
        acc = None
        for t in range(OCT // 2):
            tile = split_rows(jnp.concatenate(pieces[2 * t : 2 * t + 2], 1))
            term = jnp.dot(tile, weight[2 * width * t : 2 * width * (t + 1), :], preferred_element_type=F32)
            acc = term if acc is None else acc + term
        return fold(acc, rows_in, width)

    def level_three(start, size):
        named = [
            (box, first + blk_of(j))
            for j in range(start, start + size)
            for box, first in ((mine[j], other * blks), (theirs[j], half * blks))
        ]
        boxes = [box for box, _ in named]
        turned = [pltpu.roll(box, width // 2, 1) for box in boxes]
        pieces = []
        for o in range(OCT):
            lanes = slice(o * width, (o + 1) * width)
            cos_o, sin_o = phase[0, :, lanes], phase[1, :, lanes]
            pieces.append(
                jnp.concatenate(
                    [cos_o * box[o : o + 1, :] + sin_o * turn[o : o + 1, :] for box, turn in zip(boxes, turned)], 0
                )
            )
        result = product(pieces)
        for g, (_, index) in enumerate(named):
            three[index] = result[g * padded : (g + 1) * padded]

    def outward(k):
        @pl.when(blk + k < blks)
        def _():
            j = lax.rem(2 * blk + k + 1, blks)
            pl.semaphore_wait(ready.at[j], subs)
            each(0, subs, lambda t: copy(j * subs + t).start())

    each(1, blks, outward)

    far, near = pl.ds(0, 1), pl.ds(1, blks - 1)

    def landed(k):
        slots = got.at[pl.ds(0, subs)] if k == 0 else got.at[pl.ds(subs, (blks - 1) * subs)]
        return pltpu.make_async_copy(slots, slots, recv.at[k])

    def total(j):
        mine[j] = functools.reduce(jnp.add, [got[j * subs + t] for t in range(subs)])

    def forward(k):
        boxes = far if k == 0 else near
        return pltpu.make_async_remote_copy(
            src_ref=mine.at[boxes],
            dst_ref=theirs.at[boxes],
            send_sem=send2.at[0],
            recv_sem=recv2.at[k],
            device_id={"half": other},
            device_id_type=MESH,
        )

    landed(1).wait()
    each(1, blks, total)
    forward(1).start()
    landed(0).wait()
    total(0)
    forward(0).start()
    forward(1).wait_recv()
    for start in range(1, blks, 3):
        level_three(start, min(3, blks - start))
    forward(0).wait_recv()
    low_out[...] = theirs[lax.rem(2 * blk + 1, blks)]
    level_three(0, 1)

    for q in range(groups // OCT):
        pieces = []
        for o in range(OCT):
            lanes = slice(o * width, (o + 1) * width)
            column = q * OCT + o
            box = three[column] * keep3[:, column : column + 1]
            pieces.append(phase[2, :, lanes] * box + phase[3, :, lanes] * pltpu.roll(box, width // 2, 1))
        keep4 = jnp.sum(jnp.where(diagonal, need4[q : q + 1, :].astype(F32), 0.0), 1, keepdims=True)
        four = product(pieces) * keep4
        cone_out[:, q, :] = four[:cones]

    pltpu.make_async_copy(got, got, send.at[0]).wait()
    pltpu.make_async_copy(mine, mine, send2.at[0]).wait()


def put_out(low_ref, cone_ref, low_out, cone_out, sems):
    copies = [
        pltpu.make_async_copy(low_ref, low_out, sems.at[0]),
        pltpu.make_async_copy(cone_ref, cone_out, sems.at[1]),
    ]
    for copy in copies:
        copy.start()
    for copy in copies:
        copy.wait()


def solution(mesh):
    halves, blks, subs = mesh.shape["half"], mesh.shape["blk"], mesh.shape["sub"]
    groups = halves * blks

    def local(leaf, occupied, angles, need3, need4):
        rows, width = leaf.shape
        pairs = rows // (2 * OCT)
        per_sub = pairs // subs
        cones = need3.shape[0]
        padded = -(-cones // 8) * 8
        assert per_sub == OCT and need3.shape[1] == groups and halves == 2
        weight = jnp.asarray(weight_table(ORDER))
        lane = jnp.asarray(lane_table(ORDER))
        occupied = occupied.reshape(rows // 128, 128)
        need4 = need4.T
        vmem = pl.BlockSpec(memory_space=pltpu.VMEM)
        anywhere = pl.BlockSpec(memory_space=pl.ANY)
        results = pl.pallas_call(
            functools.partial(kernel, halves, blks, subs, cones),
            out_shape=(
                pltpu.VMEM((per_sub, width), F32),
                pltpu.VMEM((cones, groups // OCT, width), F32),
            ),
            in_specs=[anywhere] * 7,
            out_specs=(vmem, vmem),
            scratch_shapes=[
                pltpu.VMEM(leaf.shape, F32),
                pltpu.VMEM(occupied.shape, jnp.int32),
                pltpu.VMEM(angles.shape, F32),
                pltpu.VMEM(need3.shape, jnp.int32),
                pltpu.VMEM(need4.shape, jnp.int32),
                pltpu.VMEM(weight.shape, BF16),
                pltpu.VMEM(lane.shape, F32),
                pltpu.VMEM((pairs, width), F32),
                pltpu.VMEM((blks * subs, per_sub, width), F32),
                pltpu.VMEM((blks, per_sub, width), F32),
                pltpu.VMEM((blks, per_sub, width), F32),
                pltpu.VMEM((groups, padded, width), F32),
                pltpu.VMEM((4, padded, OCT * width), F32),
                pltpu.SemaphoreType.DMA((7,)),
                pltpu.SemaphoreType.DMA((1,)),
                pltpu.SemaphoreType.DMA((2,)),
                pltpu.SemaphoreType.DMA((1,)),
                pltpu.SemaphoreType.DMA((2,)),
                pltpu.SemaphoreType.REGULAR((blks,)),
            ],
            compiler_params=pltpu.CompilerParams(collective_id=0, has_side_effects=True),
            name="upward",
        )(leaf, occupied, angles, need3, need4, weight, lane)
        results = [pltpu.with_memory_space_constraint(value, pltpu.VMEM) for value in results]
        return pl.pallas_call(
            put_out,
            out_shape=[jax.ShapeDtypeStruct(value.shape, F32) for value in results],
            in_specs=[vmem] * 2,
            out_specs=[pl.BlockSpec(memory_space=pltpu.HBM)] * 2,
            scratch_shapes=[pltpu.SemaphoreType.DMA((2,))],
            name="put_out",
        )(*results)

    return jax.shard_map(
        local,
        mesh=mesh,
        in_specs=(
            P(("half", "blk", "sub"), None),
            P(("half", "blk", "sub")),
            P(),
            P(("half", "blk"), "sub"),
            P(("half", "blk"), "sub"),
        ),
        out_specs=(P(("half", "blk", "sub"), None), P(("half", "blk"), "sub", None)),
        check_vma=False,
    )
```

```python
import functools
import math
import operator

import jax
import jax.numpy as jnp
import numpy as np
from jax import lax
from jax.experimental import pallas as pl
from jax.experimental.pallas import tpu as pltpu
from jax.sharding import PartitionSpec as P

MESH = pl.DeviceIdType.MESH
F32, BF16 = jnp.float32, jnp.bfloat16
ORDER = 4
OCT = 8
NEAR = 1.5


def octant_signs():
    octant = np.arange(OCT)
    return np.stack([octant // 4 % 2, octant // 2 % 2, octant % 2], -1) * 2.0 - 1.0


def chebyshev_points(per_axis):
    return np.cos((2.0 * np.arange(per_axis) + 1.0) * math.pi / (2.0 * per_axis))


def axis_table():
    points = chebyshev_points(ORDER)
    degree = np.arange(1, ORDER)
    shifted = (points[None, :] + np.array([-1.0, 1.0])[:, None]) / 2.0
    here = np.cos(degree[None, :] * np.arccos(points)[:, None])
    there = np.cos(degree * np.arccos(shifted)[:, :, None])
    return 1.0 / ORDER + 2.0 / ORDER * np.einsum("mk,bnk->bnm", here, there)


def each(start, count, body):
    if count - start <= 64:
        for d in range(start, count):
            body(d)
    else:
        lax.fori_loop(start, count, lambda d, c: (body(d), c)[1], 0)


def split_rows(value):
    high = value.astype(BF16)
    low = (value - high.astype(F32)).astype(BF16)
    return jnp.concatenate([high, low], 0)


def fold(acc, rows, width):
    return (acc[:rows, :width] + acc[rows:, :width]) + (acc[:rows, width:] + acc[rows:, width:])


def choose(digit, values):
    return jnp.where(
        digit < 2, jnp.where(digit == 0, values[0], values[1]), jnp.where(digit == 2, values[2], values[3])
    )


def digit_of(index, place):
    return lax.rem(index // place, ORDER)


def build(table, then, bits, nodes, place):
    tile = (8, 2 * nodes)
    row, lane = lax.broadcasted_iota(jnp.int32, tile, 0), lax.broadcasted_iota(jnp.int32, tile, 1)

    def along(first, bit, i, stride):
        if bit is None:
            values = [float(table[first, i, j]) for j in range(ORDER)]
        elif isinstance(bit, int):
            values = [float(then[first, bit, i, j]) for j in range(ORDER)]
        else:
            values = [
                jnp.where(bit == 0, float(then[first, 0, i, j]), float(then[first, 1, i, j]))
                for j in range(ORDER)
            ]
        return choose(digit_of(lane, stride), values)

    bit_x, bit_y, thirds = bits
    xs = [[along(b, bit_x, i, ORDER * ORDER) for i in range(ORDER)] for b in range(2)]
    ys = [
        [jnp.where(row < ORDER, along(b, bit_y, 2 * i, ORDER), along(b, bit_y, 2 * i + 1, ORDER)) for i in range(2)]
        for b in range(2)
    ]
    zs = [
        [choose(digit_of(row, 1), [along(b, bit, i, 1) for i in range(ORDER)]) for b in range(2)] for bit in thirds
    ]
    real = lane < nodes
    for o in range(OCT):
        plane = [xs[o // 4][i // 2] * ys[o // 2 % 2][i % 2] for i in range(nodes // 8)]
        for r, third in enumerate(zs):
            block = [value * third[o % 2] for value in plane]
            wide = jnp.concatenate(
                [jnp.where(real, value, 0.0) for value in block] + [jnp.where(real, 0.0, value) for value in block], 0
            )
            high = wide.astype(BF16)
            low = (wide - high.astype(F32)).astype(BF16)
            place[pl.ds((r * OCT + o) * 2 * nodes, 2 * nodes), :] = jnp.concatenate([high, low], 1)


def product(tiles, weights):
    rows, width = tiles[0].shape
    sums = [None, None]
    for t, (tile, block) in enumerate(zip(tiles, weights)):
        term = jnp.dot(split_rows(tile), block, preferred_element_type=F32)
        sums[t % 2] = term if sums[t % 2] is None else sums[t % 2] + term
    halves = [fold(value, rows, width // 2) for value in sums if value is not None]
    return functools.reduce(jnp.add, halves)


def kernel(
    halves, blks, subs, cones,
    leaf_hbm, occ_hbm, angle_hbm, need3_hbm, need4_hbm,
    low_out, cone_out,
    leaf, occ, keep, angle, need3, need4, both, weight, part, got, mine, theirs, near, far, four,
    in_sem, send, recv, send2, recv2, ready,
):
    groups = halves * blks
    half, blk, sub = lax.axis_index("half"), lax.axis_index("blk"), lax.axis_index("sub")
    group = half * blks + blk
    pairs, family, width = leaf_hbm.shape
    nodes = width // 2
    per_sub = pairs // subs

    pltpu.make_async_copy(occ_hbm, occ, in_sem.at[0]).start()
    for q in range(family):
        pltpu.make_async_copy(leaf_hbm.at[:, q], leaf.at[pl.ds(q * pairs, pairs)], in_sem.at[1]).start()
    loads = [
        pltpu.make_async_copy(src, dst, in_sem.at[2 + i])
        for i, (src, dst) in enumerate([(angle_hbm, angle), (need3_hbm, need3), (need4_hbm, need4)])
    ]
    for load in loads:
        load.start()

    other = halves - 1 - half

    def blk_of(j):
        return lax.rem(j + blks - 1 - blk, blks)

    def sub_of(t):
        return lax.rem(t + subs - 1 - sub, subs)

    def peer(d):
        return {"half": other, "blk": blk_of(d // subs), "sub": sub_of(lax.rem(d, subs))}

    def planes(wanted, act):
        def plane(j):
            @pl.when(wanted(blk_of(j), blk))
            def _():
                each(0, subs, lambda t: act(j * subs + t))

        each(0, blks, plane)

    def greet(semaphore):
        return lambda d: pl.semaphore_signal(semaphore, inc=1, device_id=peer(d), device_id_type=MESH)

    barrier = pltpu.get_barrier_semaphore()
    planes(operator.ge, greet(barrier))

    table = axis_table()
    then = np.einsum("bij,qjk->bqik", table, table)
    build(table, then, (lax.rem(sub // 2, 2), lax.rem(sub, 2), (0, 1)), nodes, both)

    pltpu.make_async_copy(occ_hbm, occ, in_sem.at[0]).wait()
    columns = jnp.transpose(occ[...].astype(F32))
    for i in range(pairs * family // 8):
        rows8 = columns[8 * (i % 16) : 8 * (i % 16) + 8, i // 16 : i // 16 + 1]
        keep[pl.ds(i % 2 * 8 * pairs + i // 2, 8, stride=pairs), :] = jnp.broadcast_to(rows8, (8, width))
    pltpu.make_async_copy(leaf, leaf, in_sem.at[1]).wait()
    masked = [leaf[q * pairs : (q + 1) * pairs, :] * keep[q * pairs : (q + 1) * pairs, :] for q in range(family)]
    part[...] = product(
        [jnp.concatenate(masked[2 * t : 2 * t + 2], 1) for t in range(family // 2)],
        [both[2 * width * t : 2 * width * (t + 1), :] for t in range(family // 2)],
    )

    pl.semaphore_wait(barrier, (blk + 1) * subs)

    def copy(d):
        there = peer(d)
        return pltpu.make_async_remote_copy(
            src_ref=part.at[pl.ds(pl.multiple_of(there["sub"] * per_sub, 8), per_sub)],
            dst_ref=got.at[d // subs * subs + sub],
            send_sem=send.at[0],
            recv_sem=recv.at[jnp.minimum(d // subs, 1)],
            device_id=there,
            device_id_type=MESH,
        )

    planes(operator.le, lambda d: copy(d).start())
    planes(operator.lt, lambda d: greet(ready.at[d // subs])(d))

    build(table, then, (None, None, (None,)), nodes, weight)

    loads[0].wait()
    padded = near.shape[2]
    count = angle.shape[1]
    pick = lax.broadcasted_iota(jnp.int32, (padded, count), 1) == (
        lax.broadcasted_iota(jnp.int32, (padded, count), 0) + group * cones
    )
    polar = jnp.sum(jnp.where(pick, angle[0:1, :], 0.0), 1, keepdims=True)
    azimuth = jnp.sum(jnp.where(pick, angle[1:2, :], 0.0), 1, keepdims=True)
    sin_polar = jnp.sin(polar)
    direction = [sin_polar * jnp.cos(azimuth), sin_polar * jnp.sin(azimuth), jnp.cos(polar)]
    lane = lax.broadcasted_iota(jnp.int32, (padded, width), 1)
    points = [float(value) for value in chebyshev_points(ORDER)]
    places = [choose(digit_of(lane, ORDER**power), points) for power in (2, 1, 0)]
    sign = jnp.where(lane < nodes, -1.0, 1.0)
    for load in loads[1:]:
        load.wait()

    def widen(value):
        fill = padded - cones
        if fill:
            value = jnp.concatenate([value, jnp.zeros((fill, value.shape[1]), value.dtype)], 0)
        return value.astype(F32)

    keep3 = widen(need3[...])
    signs = octant_signs()
    for o in range(OCT):
        argument = sum(
            axis * (place + float(signs[o, d])) for d, (axis, place) in enumerate(zip(direction, places))
        ) * -NEAR
        cosine, sine = jnp.cos(argument), jnp.sin(argument)
        near[0, o] = cosine
        near[1, o] = sine * sign
        for g in range(o, groups, OCT):
            kept = keep3[:, g : g + 1]
            far[0, g] = (1.0 - 2.0 * sine * sine) * kept
            far[1, g] = 2.0 * sine * cosine * sign * kept
    lanes4 = need4.shape[1]
    diagonal = lax.broadcasted_iota(jnp.int32, (padded, lanes4), 0) == lax.broadcasted_iota(
        jnp.int32, (padded, lanes4), 1
    )
    keep4 = [
        jnp.sum(jnp.where(diagonal, need4[q : q + 1, :].astype(F32), 0.0), 1, keepdims=True)
        for q in range(groups // OCT)
    ]

    def outward(k):
        @pl.when(blk + k < blks)
        def _():
            j = lax.rem(2 * blk + k + 1, blks)
            pl.semaphore_wait(ready.at[j], subs)
            each(0, subs, lambda t: copy(j * subs + t).start())

    each(1, blks, outward)

    def level_three(start, size):
        boxes = [box for j in range(start, start + size) for box in (mine[j], theirs[j])]
        turned = [pltpu.roll(box, nodes, 1) for box in boxes]
        pieces = [
            jnp.concatenate(
                [near[0, o] * box[o : o + 1, :] + near[1, o] * turn[o : o + 1, :] for box, turn in zip(boxes, turned)], 0
            )
            for o in range(OCT)
        ]
        result = product(
            [jnp.concatenate(pieces[2 * t : 2 * t + 2], 1) for t in range(OCT // 2)],
            [weight[2 * width * t : 2 * width * (t + 1), :] for t in range(OCT // 2)],
        )
        index = [first + blk_of(j) for j in range(start, start + size) for first in (other * blks, half * blks)]
        return [(g, result[i * padded : (i + 1) * padded]) for i, g in enumerate(index)]

    def rows_of(g, start, size):
        base = lax.rem(g, OCT) * width + start
        return weight[pl.ds(pl.multiple_of(base, nodes), size), :]

    def level_four(found):
        turned = [far[0, g] * box + far[1, g] * pltpu.roll(box, nodes, 1) for g, box in found]
        return product(
            [jnp.concatenate(turned[i : i + 2], 1) for i in range(0, len(found), 2)],
            [
                jnp.concatenate([rows_of(g, 0, width) for g, _ in found[i : i + 2]], 0)
                for i in range(0, len(found), 2)
            ],
        )

    def level_four_last(found):
        return product(
            [jnp.concatenate([far[0, g] * box, far[1, g] * -box], 1) for g, box in found],
            [
                jnp.concatenate([rows_of(g, 0, width), rows_of(g, nodes, nodes), rows_of(g, 0, nodes)], 0)
                for g, _ in found
            ],
        )

    last, rest = pl.ds(0, 1), pl.ds(1, blks - 1)

    def landed(k):
        slots = got.at[pl.ds(0, subs)] if k == 0 else got.at[pl.ds(subs, (blks - 1) * subs)]
        return pltpu.make_async_copy(slots, slots, recv.at[k])

    def total(j):
        mine[j] = functools.reduce(jnp.add, [got[j * subs + t] for t in range(subs)])

    def forward(k):
        boxes = last if k == 0 else rest
        return pltpu.make_async_remote_copy(
            src_ref=mine.at[boxes],
            dst_ref=theirs.at[boxes],
            send_sem=send2.at[0],
            recv_sem=recv2.at[k],
            device_id={"half": other},
            device_id_type=MESH,
        )

    landed(1).wait()
    each(1, blks, total)
    forward(1).start()
    landed(0).wait()
    total(0)
    forward(0).start()
    forward(1).wait_recv()
    single = groups == OCT
    if single:
        early = level_four(level_three(1, blks - 1))
    else:
        four[...] = jnp.zeros_like(four)
        for start in range(1, blks, 3):
            for g, box in level_three(start, min(3, blks - start)):
                four[g // OCT] += level_four_last([(g, box)])
    forward(0).wait_recv()
    low_out[...] = theirs[lax.rem(2 * blk + 1, blks)]
    if single:
        cone_out[:, 0, :] = ((early + level_four_last(level_three(0, 1))) * keep4[0])[:cones]
    else:
        for g, box in level_three(0, 1):
            four[g // OCT] += level_four_last([(g, box)])
        for q in range(groups // OCT):
            cone_out[:, q, :] = (four[q] * keep4[q])[:cones]

    pltpu.make_async_copy(got, got, send.at[0]).wait()
    pltpu.make_async_copy(mine, mine, send2.at[0]).wait()


def put_out(low_ref, cone_ref, low_out, cone_out, sems):
    copies = [
        pltpu.make_async_copy(low_ref, low_out, sems.at[0]),
        pltpu.make_async_copy(cone_ref, cone_out, sems.at[1]),
    ]
    for copy in copies:
        copy.start()
    for copy in copies:
        copy.wait()


def solution(mesh):
    halves, blks, subs = mesh.shape["half"], mesh.shape["blk"], mesh.shape["sub"]
    groups = halves * blks

    def local(leaf, occupied, angles, need3, need4):
        rows, width = leaf.shape
        family = 2 * OCT
        pairs = rows // family
        per_sub = pairs // subs
        cones = need3.shape[0]
        padded = -(-cones // 8) * 8
        assert per_sub == OCT and need3.shape[1] == groups and halves == 2 and subs * 2 == OCT
        assert width == 2 * ORDER**3 and blks % 2 == 0
        leaf = leaf.reshape(pairs, family, width)
        occupied = occupied.reshape(rows // 128, 128)
        need4 = need4.T
        vmem = pl.BlockSpec(memory_space=pltpu.VMEM)
        anywhere = pl.BlockSpec(memory_space=pl.ANY)
        results = pl.pallas_call(
            functools.partial(kernel, halves, blks, subs, cones),
            out_shape=(
                pltpu.VMEM((per_sub, width), F32),
                pltpu.VMEM((cones, groups // OCT, width), F32),
            ),
            in_specs=[anywhere] * 5,
            out_specs=(vmem, vmem),
            scratch_shapes=[
                pltpu.VMEM((rows, width), F32),
                pltpu.VMEM(occupied.shape, jnp.int32),
                pltpu.VMEM((rows, width), F32),
                pltpu.VMEM(angles.shape, F32),
                pltpu.VMEM(need3.shape, jnp.int32),
                pltpu.VMEM(need4.shape, jnp.int32),
                pltpu.VMEM((family * width, 2 * width), BF16),
                pltpu.VMEM((OCT * width, 2 * width), BF16),
                pltpu.VMEM((pairs, width), F32),
                pltpu.VMEM((blks * subs, per_sub, width), F32),
                pltpu.VMEM((blks, per_sub, width), F32),
                pltpu.VMEM((blks, per_sub, width), F32),
                pltpu.VMEM((2, OCT, padded, width), F32),
                pltpu.VMEM((2, groups, padded, width), F32),
                pltpu.VMEM((groups // OCT, padded, width), F32),
                pltpu.SemaphoreType.DMA((5,)),
                pltpu.SemaphoreType.DMA((1,)),
                pltpu.SemaphoreType.DMA((2,)),
                pltpu.SemaphoreType.DMA((1,)),
                pltpu.SemaphoreType.DMA((2,)),
                pltpu.SemaphoreType.REGULAR((blks,)),
            ],
            compiler_params=pltpu.CompilerParams(collective_id=0, has_side_effects=True),
            name="upward",
        )(leaf, occupied, angles, need3, need4)
        results = [pltpu.with_memory_space_constraint(value, pltpu.VMEM) for value in results]
        return pl.pallas_call(
            put_out,
            out_shape=[jax.ShapeDtypeStruct(value.shape, F32) for value in results],
            in_specs=[vmem] * 2,
            out_specs=[pl.BlockSpec(memory_space=pltpu.HBM)] * 2,
            scratch_shapes=[pltpu.SemaphoreType.DMA((2,))],
            name="put_out",
        )(*results)

    return jax.shard_map(
        local,
        mesh=mesh,
        in_specs=(
            P(("half", "blk", "sub"), None),
            P(("half", "blk", "sub")),
            P(),
            P(("half", "blk"), "sub"),
            P(("half", "blk"), "sub"),
        ),
        out_specs=(P(("half", "blk", "sub"), None), P(("half", "blk"), "sub", None)),
        check_vma=False,
    )
```

```python
import functools
import math
import operator

import jax
import jax.numpy as jnp
import numpy as np
from jax import lax
from jax.experimental import pallas as pl
from jax.experimental.pallas import tpu as pltpu
from jax.sharding import PartitionSpec as P

MESH = pl.DeviceIdType.MESH
F32, BF16 = jnp.float32, jnp.bfloat16
ORDER = 4
OCT = 8
NEAR = 1.5


def octant_signs():
    octant = np.arange(OCT)
    return np.stack([octant // 4 % 2, octant // 2 % 2, octant % 2], -1) * 2.0 - 1.0


def chebyshev_points(per_axis):
    return np.cos((2.0 * np.arange(per_axis) + 1.0) * math.pi / (2.0 * per_axis))


def axis_table():
    points = chebyshev_points(ORDER)
    degree = np.arange(1, ORDER)
    shifted = (points[None, :] + np.array([-1.0, 1.0])[:, None]) / 2.0
    here = np.cos(degree[None, :] * np.arccos(points)[:, None])
    there = np.cos(degree * np.arccos(shifted)[:, :, None])
    return 1.0 / ORDER + 2.0 / ORDER * np.einsum("mk,bnk->bnm", here, there)


def each(start, count, body):
    if count - start <= 64:
        for d in range(start, count):
            body(d)
    else:
        lax.fori_loop(start, count, lambda d, c: (body(d), c)[1], 0)


def split_rows(value):
    high = value.astype(BF16)
    low = (value - high.astype(F32)).astype(BF16)
    return jnp.concatenate([high, low], 0)


def fold(acc, rows, width):
    return (acc[:rows, :width] + acc[rows:, :width]) + (acc[:rows, width:] + acc[rows:, width:])


def choose(digit, values):
    return jnp.where(
        digit < 2, jnp.where(digit == 0, values[0], values[1]), jnp.where(digit == 2, values[2], values[3])
    )


def digit_of(index, place):
    return lax.rem(index // place, ORDER)


def build(table, then, bits, nodes, place):
    tile = (8, 2 * nodes)
    row, lane = lax.broadcasted_iota(jnp.int32, tile, 0), lax.broadcasted_iota(jnp.int32, tile, 1)

    def along(first, bit, i, stride):
        if bit is None:
            values = [float(table[first, i, j]) for j in range(ORDER)]
        elif isinstance(bit, int):
            values = [float(then[first, bit, i, j]) for j in range(ORDER)]
        else:
            values = [
                jnp.where(bit == 0, float(then[first, 0, i, j]), float(then[first, 1, i, j]))
                for j in range(ORDER)
            ]
        return choose(digit_of(lane, stride), values)

    bit_x, bit_y, thirds = bits
    xs = [[along(b, bit_x, i, ORDER * ORDER) for i in range(ORDER)] for b in range(2)]
    ys = [
        [jnp.where(row < ORDER, along(b, bit_y, 2 * i, ORDER), along(b, bit_y, 2 * i + 1, ORDER)) for i in range(2)]
        for b in range(2)
    ]
    zs = [
        [choose(digit_of(row, 1), [along(b, bit, i, 1) for i in range(ORDER)]) for b in range(2)] for bit in thirds
    ]
    real = lane < nodes
    for o in range(OCT):
        plane = [xs[o // 4][i // 2] * ys[o // 2 % 2][i % 2] for i in range(nodes // 8)]
        for r, third in enumerate(zs):
            block = [value * third[o % 2] for value in plane]
            wide = jnp.concatenate(
                [jnp.where(real, value, 0.0) for value in block] + [jnp.where(real, 0.0, value) for value in block], 0
            )
            high = wide.astype(BF16)
            low = (wide - high.astype(F32)).astype(BF16)
            place[pl.ds((r * OCT + o) * 2 * nodes, 2 * nodes), :] = jnp.concatenate([high, low], 1)


def product(tiles, weights):
    rows, width = tiles[0].shape
    sums = [None, None]
    for t, (tile, block) in enumerate(zip(tiles, weights)):
        term = jnp.dot(split_rows(tile), block, preferred_element_type=F32)
        sums[t % 2] = term if sums[t % 2] is None else sums[t % 2] + term
    halves = [fold(value, rows, width // 2) for value in sums if value is not None]
    return functools.reduce(jnp.add, halves)


def kernel(
    halves, blks, subs, cones,
    leaf_hbm, occ_hbm, angle_hbm, need3_hbm, need4_hbm,
    low_out, cone_out,
    leaf, occ, keep, angle, need3, need4, both, weight, part, got, mine, theirs, near, far, four,
    in_sem, send, recv, recv2, ready,
):
    groups = halves * blks
    half, blk, sub = lax.axis_index("half"), lax.axis_index("blk"), lax.axis_index("sub")
    group = half * blks + blk
    pairs, family, width = leaf_hbm.shape
    nodes = width // 2
    per_sub = pairs // subs

    pltpu.make_async_copy(occ_hbm, occ, in_sem.at[0]).start()
    for q in range(family):
        pltpu.make_async_copy(leaf_hbm.at[:, q], leaf.at[pl.ds(q * pairs, pairs)], in_sem.at[1]).start()
    loads = [
        pltpu.make_async_copy(src, dst, in_sem.at[2 + i])
        for i, (src, dst) in enumerate([(angle_hbm, angle), (need3_hbm, need3), (need4_hbm, need4)])
    ]
    for load in loads:
        load.start()

    other = halves - 1 - half

    def blk_of(j):
        return lax.rem(j + blks - 1 - blk, blks)

    def sub_of(t):
        return lax.rem(t + subs - 1 - sub, subs)

    def peer(d):
        return {"half": other, "blk": blk_of(d // subs), "sub": sub_of(lax.rem(d, subs))}

    def planes(wanted, act):
        def plane(j):
            @pl.when(wanted(blk_of(j), blk))
            def _():
                each(0, subs, lambda t: act(j * subs + t))

        each(0, blks, plane)

    level = lax.rem(2 * blk + 1, blks)

    def beside(wanted, act):
        def device(t):
            @pl.when(wanted(sub_of(t), sub))
            def _():
                act(level * subs + t)

        each(0, subs, device)

    def greet(semaphore):
        return lambda d: pl.semaphore_signal(semaphore, inc=1, device_id=peer(d), device_id_type=MESH)

    def across(t):
        return {"blk": blk_of(0), "sub": sub_of(t)}

    def greet_across(semaphore):
        each(0, subs, lambda t: pl.semaphore_signal(semaphore, inc=1, device_id=across(t), device_id_type=MESH))

    is_first, is_last = blk == 0, blk == blks - 1
    is_end = lax.rem(blk, blks - 1) == 0
    barrier = pltpu.get_barrier_semaphore()
    planes(operator.gt, greet(barrier))
    beside(operator.ge, greet(barrier))

    @pl.when(is_first)
    def _():
        greet_across(barrier)

    table = axis_table()
    then = np.einsum("bij,qjk->bqik", table, table)
    build(table, then, (lax.rem(sub // 2, 2), lax.rem(sub, 2), (0, 1)), nodes, both)

    pl.semaphore_wait(barrier, (blk + is_last.astype(jnp.int32)) * subs + sub + 1)
    planes(operator.lt, lambda d: greet(ready.at[d // subs])(d))
    beside(operator.lt, greet(ready.at[level]))

    @pl.when(is_last)
    def _():
        greet_across(ready.at[0])

    pltpu.make_async_copy(occ_hbm, occ, in_sem.at[0]).wait()
    columns = jnp.transpose(occ[...].astype(F32))
    for i in range(pairs * family // 8):
        rows8 = columns[8 * (i % 16) : 8 * (i % 16) + 8, i // 16 : i // 16 + 1]
        keep[pl.ds(i % 2 * 8 * pairs + i // 2, 8, stride=pairs), :] = jnp.broadcast_to(rows8, (8, width))
    pltpu.make_async_copy(leaf, leaf, in_sem.at[1]).wait()
    masked = [leaf[q * pairs : (q + 1) * pairs, :] * keep[q * pairs : (q + 1) * pairs, :] for q in range(family)]
    part[...] = product(
        [jnp.concatenate(masked[2 * t : 2 * t + 2], 1) for t in range(family // 2)],
        [both[2 * width * t : 2 * width * (t + 1), :] for t in range(family // 2)],
    )


    def copy(d, there=None):
        there = peer(d) if there is None else there
        j = d // subs
        return pltpu.make_async_remote_copy(
            src_ref=part.at[pl.ds(pl.multiple_of(there["sub"] * per_sub, 8), per_sub)],
            dst_ref=got.at[jnp.where(j == 0, half, j + 1) * subs + sub],
            send_sem=send.at[0],
            recv_sem=recv.at[jnp.minimum(j, 1)],
            device_id=there,
            device_id_type=MESH,
        )

    def copy_across():
        for to in range(halves):
            each(0, subs, lambda t: copy(t, {"half": to, **across(t)}).start())

    pl.when(is_last)(copy_across)
    def inward(there):
        @pl.when(jnp.logical_and(there < blk, there + blks - 1 != blk))
        def _():
            j = lax.rem(blk + there + 1, blks)
            each(0, subs, lambda t: copy(j * subs + t).start())

    each(0, blks - 1, inward)
    beside(operator.le, lambda d: copy(d).start())

    build(table, then, (None, None, (None,)), nodes, weight)

    loads[0].wait()
    padded = near.shape[2]
    count = angle.shape[1]
    pick = lax.broadcasted_iota(jnp.int32, (padded, count), 1) == (
        lax.broadcasted_iota(jnp.int32, (padded, count), 0) + group * cones
    )
    polar = jnp.sum(jnp.where(pick, angle[0:1, :], 0.0), 1, keepdims=True)
    azimuth = jnp.sum(jnp.where(pick, angle[1:2, :], 0.0), 1, keepdims=True)
    sin_polar = jnp.sin(polar)
    direction = [sin_polar * jnp.cos(azimuth), sin_polar * jnp.sin(azimuth), jnp.cos(polar)]
    lane = lax.broadcasted_iota(jnp.int32, (padded, width), 1)
    points = [float(value) for value in chebyshev_points(ORDER)]
    places = [choose(digit_of(lane, ORDER**power), points) for power in (2, 1, 0)]
    sign = jnp.where(lane < nodes, -1.0, 1.0)
    for load in loads[1:]:
        load.wait()

    def widen(value):
        fill = padded - cones
        if fill:
            value = jnp.concatenate([value, jnp.zeros((fill, value.shape[1]), value.dtype)], 0)
        return value.astype(F32)

    keep3 = widen(need3[...])
    signs = octant_signs()
    for o in range(OCT):
        argument = sum(
            axis * (place + float(signs[o, d])) for d, (axis, place) in enumerate(zip(direction, places))
        ) * -NEAR
        cosine, sine = jnp.cos(argument), jnp.sin(argument)
        near[0, o] = cosine
        near[1, o] = sine * sign
        for g in range(o, groups, OCT):
            kept = keep3[:, g : g + 1]
            far[0, g] = (1.0 - 2.0 * sine * sine) * kept
            far[1, g] = 2.0 * sine * cosine * sign * kept
    lanes4 = need4.shape[1]
    diagonal = lax.broadcasted_iota(jnp.int32, (padded, lanes4), 0) == lax.broadcasted_iota(
        jnp.int32, (padded, lanes4), 1
    )
    keep4 = [
        jnp.sum(jnp.where(diagonal, need4[q : q + 1, :].astype(F32), 0.0), 1, keepdims=True)
        for q in range(groups // OCT)
    ]

    def outward(k):
        @pl.when(blk + k < blks)
        def _():
            if k == blks - 1:
                pl.semaphore_wait(ready.at[0], halves * subs)
                copy_across()
            else:
                j = lax.rem(2 * blk + k + 1, blks)
                pl.semaphore_wait(ready.at[j], subs)
                each(0, subs, lambda t: copy(j * subs + t).start())

    @pl.when(sub < subs - 1)
    def _():
        pl.semaphore_wait(ready.at[level], subs - 1 - sub)
        beside(operator.gt, lambda d: copy(d).start())

    each(1, blks, outward)

    def level_three(places):
        boxes = [(mine, theirs)[own][j] for own, j in places]
        turned = [pltpu.roll(box, nodes, 1) for box in boxes]
        pieces = [
            jnp.concatenate(
                [near[0, o] * box[o : o + 1, :] + near[1, o] * turn[o : o + 1, :] for box, turn in zip(boxes, turned)], 0
            )
            for o in range(OCT)
        ]
        result = product(
            [jnp.concatenate(pieces[2 * t : 2 * t + 2], 1) for t in range(OCT // 2)],
            [weight[2 * width * t : 2 * width * (t + 1), :] for t in range(OCT // 2)],
        )
        index = [(other, half)[own] * blks + blk_of(j) for own, j in places]
        return [(g, result[i * padded : (i + 1) * padded]) for i, g in enumerate(index)]

    def rows_of(g, start, size):
        base = lax.rem(g, OCT) * width + start
        return weight[pl.ds(pl.multiple_of(base, nodes), size), :]

    def level_four(found):
        return product(
            [jnp.concatenate([far[0, g] * box, far[1, g] * -box], 1) for g, box in found],
            [
                jnp.concatenate([rows_of(g, 0, width), rows_of(g, nodes, nodes), rows_of(g, 0, nodes)], 0)
                for g, _ in found
            ],
        )

    last, rest = pl.ds(0, 1), pl.ds(1, blks - 1)

    def landed(semaphore, first, count):
        slots = got.at[pl.ds(first * subs, count * subs)]
        pltpu.make_async_copy(slots, slots, semaphore).wait()

    def total(slot):
        return functools.reduce(jnp.add, [got[slot * subs + t] for t in range(subs)])

    def forward(k):
        boxes = last if k == 0 else rest
        return pltpu.make_async_remote_copy(
            src_ref=mine.at[boxes],
            dst_ref=theirs.at[boxes],
            send_sem=send.at[0],
            recv_sem=recv2.at[0],
            device_id={"half": other},
            device_id_type=MESH,
        )

    landed(recv.at[1], halves, blks - 1)
    for j in range(1, blks):
        mine[j] = total(j + 1)
    forward(1).start()

    @pl.when(jnp.logical_not(is_end))
    def _():
        landed(recv.at[0], other, 1)
        mine[0] = total(other)
        forward(0).start()

    single = groups == OCT
    direct = [(0, j) for j in range(1, blks)]
    handed = [(1, j) for j in range(1, blks)] + [(0, 0), (1, 0)]
    if single:
        early = level_four(level_three(direct))

    def handed_over(boxes):
        pltpu.make_async_copy(theirs.at[boxes], theirs.at[boxes], recv2.at[0]).wait()

    @pl.when(is_end)
    def _():
        handed_over(rest)
        landed(recv.at[0], 0, halves)
        mine[0] = total(other)
        theirs[0] = total(half)

    @pl.when(jnp.logical_not(is_end))
    def _():
        handed_over(pl.ds(0, blks))

    if single:
        cone_out[:, 0, :] = ((early + level_four(level_three(handed))) * keep4[0])[:cones]
    else:
        four[...] = jnp.zeros_like(four)
        together = direct + handed
        for start in range(0, len(together), 6):
            for g, box in level_three(together[start : start + 6]):
                four[g // OCT] += level_four([(g, box)])
        for q in range(groups // OCT):
            cone_out[:, q, :] = (four[q] * keep4[q])[:cones]
    low_out[...] = theirs[level]

    def sent(count):
        slots = got.at[pl.ds(0, count)]
        pltpu.make_async_copy(slots, slots, send.at[0]).wait()

    @pl.when(is_end)
    def _():
        sent((blks + 1) * subs + blks - 1)

    @pl.when(jnp.logical_not(is_end))
    def _():
        sent(blks * subs + blks)


def put_out(low_ref, cone_ref, low_out, cone_out, sems):
    copies = [
        pltpu.make_async_copy(low_ref, low_out, sems.at[0]),
        pltpu.make_async_copy(cone_ref, cone_out, sems.at[1]),
    ]
    for copy in copies:
        copy.start()
    for copy in copies:
        copy.wait()


def solution(mesh):
    halves, blks, subs = mesh.shape["half"], mesh.shape["blk"], mesh.shape["sub"]
    groups = halves * blks

    def local(leaf, occupied, angles, need3, need4):
        rows, width = leaf.shape
        family = 2 * OCT
        pairs = rows // family
        per_sub = pairs // subs
        cones = need3.shape[0]
        padded = -(-cones // 8) * 8
        assert per_sub == OCT and need3.shape[1] == groups and halves == 2 and subs * 2 == OCT
        assert width == 2 * ORDER**3 and blks % 2 == 0
        leaf = leaf.reshape(pairs, family, width)
        occupied = occupied.reshape(rows // 128, 128)
        need4 = need4.T
        vmem = pl.BlockSpec(memory_space=pltpu.VMEM)
        anywhere = pl.BlockSpec(memory_space=pl.ANY)
        results = pl.pallas_call(
            functools.partial(kernel, halves, blks, subs, cones),
            out_shape=(
                pltpu.VMEM((per_sub, width), F32),
                pltpu.VMEM((cones, groups // OCT, width), F32),
            ),
            in_specs=[anywhere] * 5,
            out_specs=(vmem, vmem),
            scratch_shapes=[
                pltpu.VMEM((rows, width), F32),
                pltpu.VMEM(occupied.shape, jnp.int32),
                pltpu.VMEM((rows, width), F32),
                pltpu.VMEM(angles.shape, F32),
                pltpu.VMEM(need3.shape, jnp.int32),
                pltpu.VMEM(need4.shape, jnp.int32),
                pltpu.VMEM((family * width, 2 * width), BF16),
                pltpu.VMEM((OCT * width, 2 * width), BF16),
                pltpu.VMEM((pairs, width), F32),
                pltpu.VMEM(((blks + 1) * subs + blks, per_sub, width), F32),
                pltpu.VMEM((blks, per_sub, width), F32),
                pltpu.VMEM((blks, per_sub, width), F32),
                pltpu.VMEM((2, OCT, padded, width), F32),
                pltpu.VMEM((2, groups, padded, width), F32),
                pltpu.VMEM((groups // OCT, padded, width), F32),
                pltpu.SemaphoreType.DMA((5,)),
                pltpu.SemaphoreType.DMA((1,)),
                pltpu.SemaphoreType.DMA((2,)),
                pltpu.SemaphoreType.DMA((1,)),
                pltpu.SemaphoreType.REGULAR((blks,)),
            ],
            compiler_params=pltpu.CompilerParams(collective_id=0, has_side_effects=True),
            name="upward",
        )(leaf, occupied, angles, need3, need4)
        results = [pltpu.with_memory_space_constraint(value, pltpu.VMEM) for value in results]
        return pl.pallas_call(
            put_out,
            out_shape=[jax.ShapeDtypeStruct(value.shape, F32) for value in results],
            in_specs=[vmem] * 2,
            out_specs=[pl.BlockSpec(memory_space=pltpu.HBM)] * 2,
            scratch_shapes=[pltpu.SemaphoreType.DMA((2,))],
            name="put_out",
        )(*results)

    return jax.shard_map(
        local,
        mesh=mesh,
        in_specs=(
            P(("half", "blk", "sub"), None),
            P(("half", "blk", "sub")),
            P(),
            P(("half", "blk"), "sub"),
            P(("half", "blk"), "sub"),
        ),
        out_specs=(P(("half", "blk", "sub"), None), P(("half", "blk"), "sub", None)),
        check_vma=False,
    )
```

```python
import functools
import math
import operator

import jax
import jax.numpy as jnp
import numpy as np
from jax import lax
from jax.experimental import pallas as pl
from jax.experimental.pallas import tpu as pltpu
from jax.sharding import PartitionSpec as P

MESH = pl.DeviceIdType.MESH
F32, BF16 = jnp.float32, jnp.bfloat16
ORDER = 4
OCT = 8
NEAR = 1.5


def octant_signs():
    octant = np.arange(OCT)
    return np.stack([octant // 4 % 2, octant // 2 % 2, octant % 2], -1) * 2.0 - 1.0


def chebyshev_points(per_axis):
    return np.cos((2.0 * np.arange(per_axis) + 1.0) * math.pi / (2.0 * per_axis))


def axis_table():
    points = chebyshev_points(ORDER)
    degree = np.arange(1, ORDER)
    shifted = (points[None, :] + np.array([-1.0, 1.0])[:, None]) / 2.0
    here = np.cos(degree[None, :] * np.arccos(points)[:, None])
    there = np.cos(degree * np.arccos(shifted)[:, :, None])
    return 1.0 / ORDER + 2.0 / ORDER * np.einsum("mk,bnk->bnm", here, there)


def each(start, count, body):
    if count - start <= 64:
        for d in range(start, count):
            body(d)
    else:
        lax.fori_loop(start, count, lambda d, c: (body(d), c)[1], 0)


def split_rows(value):
    high = value.astype(BF16).astype(F32)
    return jnp.concatenate([high, value - high], 0).astype(BF16)


def fold(acc, rows, width):
    return (acc[:rows, :width] + acc[rows:, :width]) + (acc[:rows, width:] + acc[rows:, width:])


def choose(digit, values):
    return jnp.where(
        digit < 2, jnp.where(digit == 0, values[0], values[1]), jnp.where(digit == 2, values[2], values[3])
    )


def digit_of(index, place):
    return lax.rem(index // place, ORDER)


def build(table, then, bits, nodes, place):
    tile = (8, 2 * nodes)
    row, lane = lax.broadcasted_iota(jnp.int32, tile, 0), lax.broadcasted_iota(jnp.int32, tile, 1)

    def along(first, bit, i, stride):
        if bit is None:
            values = [float(table[first, i, j]) for j in range(ORDER)]
        elif isinstance(bit, int):
            values = [float(then[first, bit, i, j]) for j in range(ORDER)]
        else:
            values = [
                jnp.where(bit == 0, float(then[first, 0, i, j]), float(then[first, 1, i, j]))
                for j in range(ORDER)
            ]
        return choose(digit_of(lane, stride), values)

    bit_x, bit_y, thirds = bits
    xs = [[along(b, bit_x, i, ORDER * ORDER) for i in range(ORDER)] for b in range(2)]
    ys = [
        [jnp.where(row < ORDER, along(b, bit_y, 2 * i, ORDER), along(b, bit_y, 2 * i + 1, ORDER)) for i in range(2)]
        for b in range(2)
    ]
    zs = [
        [choose(digit_of(row, 1), [along(b, bit, i, 1) for i in range(ORDER)]) for b in range(2)] for bit in thirds
    ]
    real = lane < nodes
    for o in range(OCT):
        plane = [xs[o // 4][i // 2] * ys[o // 2 % 2][i % 2] for i in range(nodes // 8)]
        for r, third in enumerate(zs):
            block = [value * third[o % 2] for value in plane]
            wide = jnp.concatenate(
                [jnp.where(real, value, 0.0) for value in block] + [jnp.where(real, 0.0, value) for value in block], 0
            )
            high = wide.astype(BF16)
            low = (wide - high.astype(F32)).astype(BF16)
            place[pl.ds((r * OCT + o) * 2 * nodes, 2 * nodes), :] = jnp.concatenate([high, low], 1)


def push(weights, t, register):
    pltpu.matmul_push_rhs(weights(t), staging_register=register, mxu_index=t % 2)


def stage(sums, weights):
    for t in range(2):
        push(weights, t, 0)
        pltpu.matmul_acc_lhs(sums[t], jnp.zeros(sums[t].shape, BF16), load_staged_rhs=0)
    for t in range(2, 6):
        push(weights, t, t // 2 - 1)


def staged_product(sums, tiles, weights):
    for t, tile in enumerate(tiles):
        pltpu.matmul_acc_lhs(sums[t % 2], split_rows(tile), load_staged_rhs=(None, 0, 1, 0)[t // 2])
        if t // 2 == 1:
            push(weights, t + 4, 0)
    return collect(sums, tiles)


def product(sums, tiles, weights):
    for t, tile in enumerate(tiles):
        push(weights, t, t // 2 % 2)
        pltpu.matmul_acc_lhs(sums[t % 2], split_rows(tile), load_staged_rhs=t // 2 % 2)
    return collect(sums, tiles)


def collect(sums, tiles):
    rows, width = tiles[0].shape
    parts = [fold(pltpu.matmul_pop(total), rows, width // 2) for total in sums[: len(tiles)]]
    return functools.reduce(jnp.add, parts)


def kernel(halves, blks, subs, cones, sizes, *refs):
    specs = [pltpu.ACC(unit)((rows, 2 * refs[0].shape[-1]), F32) for rows in sizes for unit in range(2)]

    def inside(*totals):
        for total in totals:
            pltpu.matmul_pop(total)
        sums = {rows: totals[2 * i : 2 * i + 2] for i, rows in enumerate(sizes)}
        upward(halves, blks, subs, cones, sums, *refs)

    pl.run_scoped(inside, *specs)


def upward(
    halves, blks, subs, cones, sums,
    leaf_hbm, occ_hbm, angle_hbm, need3_hbm, need4_hbm,
    low_out, cone_out,
    leaf, occ, keep, angle, need3, need4, both, weight, part, got, mine, theirs, near, far, four,
    in_sem, send, recv, recv2, ready,
):
    groups = halves * blks
    half, blk, sub = lax.axis_index("half"), lax.axis_index("blk"), lax.axis_index("sub")
    group = half * blks + blk
    pairs, family, width = leaf_hbm.shape
    nodes = width // 2
    per_sub = pairs // subs

    pltpu.make_async_copy(occ_hbm, occ, in_sem.at[0]).start()
    for q in range(family):
        pltpu.make_async_copy(leaf_hbm.at[:, q], leaf.at[pl.ds(q * pairs, pairs)], in_sem.at[1]).start()
    loads = [
        pltpu.make_async_copy(src, dst, in_sem.at[2 + i])
        for i, (src, dst) in enumerate([(angle_hbm, angle), (need3_hbm, need3), (need4_hbm, need4)])
    ]
    for load in loads:
        load.start()

    other = halves - 1 - half

    def blk_of(j):
        return lax.rem(j + blks - 1 - blk, blks)

    def sub_of(t):
        return lax.rem(t + subs - 1 - sub, subs)

    def peer(d):
        return {"half": other, "blk": blk_of(d // subs), "sub": sub_of(lax.rem(d, subs))}

    def planes(wanted, act):
        def plane(j):
            @pl.when(wanted(blk_of(j), blk))
            def _():
                each(0, subs, lambda t: act(j * subs + t))

        each(0, blks, plane)

    level = lax.rem(2 * blk + 1, blks)

    def beside(wanted, act):
        def device(t):
            @pl.when(wanted(sub_of(t), sub))
            def _():
                act(level * subs + t)

        each(0, subs, device)

    def greet(semaphore):
        return lambda d: pl.semaphore_signal(semaphore, inc=1, device_id=peer(d), device_id_type=MESH)

    def across(t):
        return {"blk": blk_of(0), "sub": sub_of(t)}

    def greet_across(semaphore):
        each(0, subs, lambda t: pl.semaphore_signal(semaphore, inc=1, device_id=across(t), device_id_type=MESH))

    is_first, is_last = blk == 0, blk == blks - 1
    is_end = lax.rem(blk, blks - 1) == 0
    barrier = pltpu.get_barrier_semaphore()
    planes(operator.gt, greet(barrier))
    beside(operator.ge, greet(barrier))

    @pl.when(is_first)
    def _():
        greet_across(barrier)

    table = axis_table()
    then = np.einsum("bij,qjk->bqik", table, table)
    build(table, then, (lax.rem(sub // 2, 2), lax.rem(sub, 2), (0, 1)), nodes, both)

    pl.semaphore_wait(barrier, (blk + is_last.astype(jnp.int32)) * subs + sub + 1)

    @pl.when(is_last)
    def _():
        greet_across(ready.at[0])

    planes(operator.lt, lambda d: greet(ready.at[d // subs])(d))
    beside(operator.lt, greet(ready.at[level]))
    pltpu.make_async_copy(occ_hbm, occ, in_sem.at[0]).wait()
    columns = jnp.transpose(occ[...].astype(F32))
    for i in range(pairs * family // 8):
        rows8 = columns[8 * (i % 16) : 8 * (i % 16) + 8, i // 16 : i // 16 + 1]
        keep[pl.ds(i % 2 * 8 * pairs + i // 2, 8, stride=pairs), :] = jnp.broadcast_to(rows8, (8, width))
    def first_weights(t):
        return both[2 * width * t : 2 * width * (t + 1), :]

    stage(sums[2 * pairs], first_weights)
    pltpu.make_async_copy(leaf, leaf, in_sem.at[1]).wait()
    masked = [leaf[q * pairs : (q + 1) * pairs, :] * keep[q * pairs : (q + 1) * pairs, :] for q in range(family)]
    part[...] = staged_product(
        sums[2 * pairs], [jnp.concatenate(masked[2 * t : 2 * t + 2], 1) for t in range(family // 2)], first_weights
    )

    def copy(d, there=None):
        there = peer(d) if there is None else there
        j = d // subs
        return pltpu.make_async_remote_copy(
            src_ref=part.at[pl.ds(pl.multiple_of(there["sub"] * per_sub, 8), per_sub)],
            dst_ref=got.at[jnp.where(j == 0, half, j + 1) * subs + sub],
            send_sem=send.at[0],
            recv_sem=recv.at[jnp.minimum(j, 1)],
            device_id=there,
            device_id_type=MESH,
        )

    def copy_across(order):
        for to in order:
            each(0, subs, lambda t: copy(t, {"half": to, **across(t)}).start())

    @pl.when(is_last)
    def _():
        copy_across(range(halves))

    def inward(there):
        @pl.when(jnp.logical_and(there < blk, there + blks - 1 != blk))
        def _():
            j = lax.rem(blk + there + 1, blks)
            each(0, subs, lambda t: copy(j * subs + t).start())

    each(0, blks - 1, inward)
    beside(operator.le, lambda d: copy(d).start())

    build(table, then, (None, None, (None,)), nodes, weight)

    loads[0].wait()
    padded = near.shape[2]
    count = angle.shape[1]
    pick = lax.broadcasted_iota(jnp.int32, (padded, count), 1) == (
        lax.broadcasted_iota(jnp.int32, (padded, count), 0) + group * cones
    )
    polar = jnp.sum(jnp.where(pick, angle[0:1, :], 0.0), 1, keepdims=True)
    azimuth = jnp.sum(jnp.where(pick, angle[1:2, :], 0.0), 1, keepdims=True)
    sin_polar = jnp.sin(polar)
    direction = [sin_polar * jnp.cos(azimuth), sin_polar * jnp.sin(azimuth), jnp.cos(polar)]
    lane = lax.broadcasted_iota(jnp.int32, (padded, width), 1)
    points = [float(value) for value in chebyshev_points(ORDER)]
    places = [choose(digit_of(lane, ORDER**power), points) for power in (2, 1, 0)]
    sign = jnp.where(lane < nodes, -1.0, 1.0)
    for load in loads[1:]:
        load.wait()

    def widen(value):
        fill = padded - cones
        if fill:
            value = jnp.concatenate([value, jnp.zeros((fill, value.shape[1]), value.dtype)], 0)
        return value.astype(F32)

    keep3 = widen(need3[...])
    signs = octant_signs()
    for o in range(OCT):
        argument = sum(
            axis * (place + float(signs[o, d])) for d, (axis, place) in enumerate(zip(direction, places))
        ) * -NEAR
        cosine, sine = jnp.cos(argument), jnp.sin(argument)
        near[0, o] = cosine
        near[1, o] = sine * sign
        for g in range(o, groups, OCT):
            kept = keep3[:, g : g + 1]
            far[0, g] = (1.0 - 2.0 * sine * sine) * kept
            far[1, g] = 2.0 * sine * cosine * sign * kept
    lanes4 = need4.shape[1]
    diagonal = lax.broadcasted_iota(jnp.int32, (padded, lanes4), 0) == lax.broadcasted_iota(
        jnp.int32, (padded, lanes4), 1
    )
    keep4 = [
        jnp.sum(jnp.where(diagonal, need4[q : q + 1, :].astype(F32), 0.0), 1, keepdims=True)
        for q in range(groups // OCT)
    ]

    def outward(k):
        @pl.when(blk + k < blks)
        def _():
            if k == blks - 1:
                pl.semaphore_wait(ready.at[0], halves * subs)
                copy_across(reversed(range(halves)))
            else:
                j = lax.rem(2 * blk + k + 1, blks)
                pl.semaphore_wait(ready.at[j], subs)
                each(0, subs, lambda t: copy(j * subs + t).start())

    @pl.when(sub < subs - 1)
    def _():
        pl.semaphore_wait(ready.at[level], subs - 1 - sub)
        beside(operator.gt, lambda d: copy(d).start())

    each(1, blks, outward)

    def rows_of(base, start, size):
        return weight[pl.ds(pl.multiple_of(base + start, nodes), size), :]

    def turning(o):
        base = lax.rem(o, OCT) * width
        return jnp.concatenate([rows_of(base, 0, width), rows_of(base, nodes, nodes), rows_of(base, 0, nodes)], 0)

    def level_three(places, multiply):
        boxes = [(mine, theirs)[own][j] for own, j in places]
        tiles = [
            jnp.concatenate(
                [
                    jnp.concatenate([near[0, o] * box[o : o + 1, :], near[1, o] * -box[o : o + 1, :]], 1)
                    for box in boxes
                ],
                0,
            )
            for o in range(OCT)
        ]
        result = multiply(sums[2 * padded * len(places)], tiles, turning)
        index = [(other, half)[own] * blks + blk_of(j) for own, j in places]
        return [(g, result[i * padded : (i + 1) * padded]) for i, g in enumerate(index)]

    def level_four(found):
        tiles = [jnp.concatenate([far[0, g] * box, far[1, g] * -box], 1) for g, box in found]
        return product(sums[2 * padded], tiles, lambda t: turning(found[t][0]))

    last, rest = pl.ds(0, 1), pl.ds(1, blks - 1)

    def landed(semaphore, first, count):
        slots = got.at[pl.ds(first * subs, count * subs)]
        pltpu.make_async_copy(slots, slots, semaphore).wait()

    def total(slot):
        return functools.reduce(jnp.add, [got[slot * subs + t] for t in range(subs)])

    def forward(k):
        boxes = last if k == 0 else rest
        return pltpu.make_async_remote_copy(
            src_ref=mine.at[boxes],
            dst_ref=theirs.at[boxes],
            send_sem=send.at[0],
            recv_sem=recv2.at[0],
            device_id={"half": other},
            device_id_type=MESH,
        )

    landed(recv.at[1], halves, blks - 1)
    for j in range(1, blks):
        mine[j] = total(j + 1)
    forward(1).start()

    @pl.when(jnp.logical_not(is_end))
    def _():
        landed(recv.at[0], other, 1)
        mine[0] = total(other)
        forward(0).start()

    single = groups == OCT
    direct = [(0, j) for j in range(1, blks)]
    handed = [(1, j) for j in range(1, blks)] + [(0, 0), (1, 0)]
    if single:
        early = level_four(level_three(direct, product))
        stage(sums[2 * padded * len(handed)], turning)

    def handed_over(boxes):
        pltpu.make_async_copy(theirs.at[boxes], theirs.at[boxes], recv2.at[0]).wait()

    @pl.when(is_end)
    def _():
        handed_over(rest)
        landed(recv.at[0], 0, halves)
        mine[0] = total(other)
        theirs[0] = total(half)

    @pl.when(jnp.logical_not(is_end))
    def _():
        handed_over(pl.ds(0, blks))

    if single:
        cone_out[:, 0, :] = ((early + level_four(level_three(handed, staged_product))) * keep4[0])[:cones]
    else:
        four[...] = jnp.zeros_like(four)
        together = direct + handed
        for start in range(0, len(together), 6):
            for g, box in level_three(together[start : start + 6], product):
                four[g // OCT] += level_four([(g, box)])
        for q in range(groups // OCT):
            cone_out[:, q, :] = (four[q] * keep4[q])[:cones]
    low_out[...] = theirs[level]

    def sent(count):
        slots = got.at[pl.ds(0, count)]
        pltpu.make_async_copy(slots, slots, send.at[0]).wait()

    @pl.when(is_end)
    def _():
        sent((blks + 1) * subs + blks - 1)

    @pl.when(jnp.logical_not(is_end))
    def _():
        sent(blks * subs + blks)


def put_out(low_ref, cone_ref, low_out, cone_out, sems):
    copies = [
        pltpu.make_async_copy(low_ref, low_out, sems.at[0]),
        pltpu.make_async_copy(cone_ref, cone_out, sems.at[1]),
    ]
    for copy in copies:
        copy.start()
    for copy in copies:
        copy.wait()


def solution(mesh):
    halves, blks, subs = mesh.shape["half"], mesh.shape["blk"], mesh.shape["sub"]
    groups = halves * blks

    def local(leaf, occupied, angles, need3, need4):
        rows, width = leaf.shape
        family = 2 * OCT
        pairs = rows // family
        per_sub = pairs // subs
        cones = need3.shape[0]
        padded = -(-cones // 8) * 8
        assert per_sub == OCT and need3.shape[1] == groups and halves == 2 and subs * 2 == OCT
        assert width == 2 * ORDER**3 and blks % 2 == 0
        boxes = (blks - 1, blks + 1) if groups == OCT else (6, 2 * blks % 6)
        sizes = sorted({2 * pairs, 2 * padded} | {2 * padded * count for count in boxes if count})
        leaf = leaf.reshape(pairs, family, width)
        occupied = occupied.reshape(rows // 128, 128)
        need4 = need4.T
        vmem = pl.BlockSpec(memory_space=pltpu.VMEM)
        anywhere = pl.BlockSpec(memory_space=pl.ANY)
        results = pl.pallas_call(
            functools.partial(kernel, halves, blks, subs, cones, sizes),
            out_shape=(
                pltpu.VMEM((per_sub, width), F32),
                pltpu.VMEM((cones, groups // OCT, width), F32),
            ),
            in_specs=[anywhere] * 5,
            out_specs=(vmem, vmem),
            scratch_shapes=[
                pltpu.VMEM((rows, width), F32),
                pltpu.VMEM(occupied.shape, jnp.int32),
                pltpu.VMEM((rows, width), F32),
                pltpu.VMEM(angles.shape, F32),
                pltpu.VMEM(need3.shape, jnp.int32),
                pltpu.VMEM(need4.shape, jnp.int32),
                pltpu.VMEM((family * width, 2 * width), BF16),
                pltpu.VMEM((OCT * width, 2 * width), BF16),
                pltpu.VMEM((pairs, width), F32),
                pltpu.VMEM(((blks + 1) * subs + blks, per_sub, width), F32),
                pltpu.VMEM((blks, per_sub, width), F32),
                pltpu.VMEM((blks, per_sub, width), F32),
                pltpu.VMEM((2, OCT, padded, width), F32),
                pltpu.VMEM((2, groups, padded, width), F32),
                pltpu.VMEM((groups // OCT, padded, width), F32),
                pltpu.SemaphoreType.DMA((5,)),
                pltpu.SemaphoreType.DMA((1,)),
                pltpu.SemaphoreType.DMA((2,)),
                pltpu.SemaphoreType.DMA((1,)),
                pltpu.SemaphoreType.REGULAR((blks,)),
            ],
            compiler_params=pltpu.CompilerParams(collective_id=0, has_side_effects=True),
            name="upward",
        )(leaf, occupied, angles, need3, need4)
        results = [pltpu.with_memory_space_constraint(value, pltpu.VMEM) for value in results]
        return pl.pallas_call(
            put_out,
            out_shape=[jax.ShapeDtypeStruct(value.shape, F32) for value in results],
            in_specs=[vmem] * 2,
            out_specs=[pl.BlockSpec(memory_space=pltpu.HBM)] * 2,
            scratch_shapes=[pltpu.SemaphoreType.DMA((2,))],
            name="put_out",
        )(*results)

    return jax.shard_map(
        local,
        mesh=mesh,
        in_specs=(
            P(("half", "blk", "sub"), None),
            P(("half", "blk", "sub")),
            P(),
            P(("half", "blk"), "sub"),
            P(("half", "blk"), "sub"),
        ),
        out_specs=(P(("half", "blk", "sub"), None), P(("half", "blk"), "sub", None)),
        check_vma=False,
    )
```

```python
import functools
import math
import operator

import jax
import jax.numpy as jnp
import numpy as np
from jax import lax
from jax.experimental import pallas as pl
from jax.experimental.pallas import tpu as pltpu
from jax.sharding import PartitionSpec as P

MESH = pl.DeviceIdType.MESH
F32, BF16 = jnp.float32, jnp.bfloat16
ORDER = 4
OCT = 8
NEAR = 1.5


def octant_signs():
    octant = np.arange(OCT)
    return np.stack([octant // 4 % 2, octant // 2 % 2, octant % 2], -1) * 2.0 - 1.0


def chebyshev_points(per_axis):
    return np.cos((2.0 * np.arange(per_axis) + 1.0) * math.pi / (2.0 * per_axis))


def axis_table():
    points = chebyshev_points(ORDER)
    degree = np.arange(1, ORDER)
    shifted = (points[None, :] + np.array([-1.0, 1.0])[:, None]) / 2.0
    here = np.cos(degree[None, :] * np.arccos(points)[:, None])
    there = np.cos(degree * np.arccos(shifted)[:, :, None])
    return 1.0 / ORDER + 2.0 / ORDER * np.einsum("mk,bnk->bnm", here, there)


def each(start, count, body):
    if count - start <= 64:
        for d in range(start, count):
            body(d)
    else:
        lax.fori_loop(start, count, lambda d, c: (body(d), c)[1], 0)


def split_rows(value):
    high = value.astype(BF16).astype(F32)
    return jnp.concatenate([high, value - high], 0).astype(BF16)


def fold(acc, rows, width):
    return (acc[:rows, :width] + acc[rows:, :width]) + (acc[:rows, width:] + acc[rows:, width:])


def choose(digit, values):
    return jnp.where(
        digit < 2, jnp.where(digit == 0, values[0], values[1]), jnp.where(digit == 2, values[2], values[3])
    )


def digit_of(index, place):
    return lax.rem(index // place, ORDER)


def build(table, then, bits, nodes, place):
    tile = (8, 2 * nodes)
    row, lane = lax.broadcasted_iota(jnp.int32, tile, 0), lax.broadcasted_iota(jnp.int32, tile, 1)

    def along(first, bit, i, stride):
        if bit is None:
            values = [float(table[first, i, j]) for j in range(ORDER)]
        elif isinstance(bit, int):
            values = [float(then[first, bit, i, j]) for j in range(ORDER)]
        else:
            values = [
                jnp.where(bit == 0, float(then[first, 0, i, j]), float(then[first, 1, i, j]))
                for j in range(ORDER)
            ]
        return choose(digit_of(lane, stride), values)

    bit_x, bit_y, thirds = bits
    xs = [[along(b, bit_x, i, ORDER * ORDER) for i in range(ORDER)] for b in range(2)]
    ys = [
        [jnp.where(row < ORDER, along(b, bit_y, 2 * i, ORDER), along(b, bit_y, 2 * i + 1, ORDER)) for i in range(2)]
        for b in range(2)
    ]
    zs = [
        [choose(digit_of(row, 1), [along(b, bit, i, 1) for i in range(ORDER)]) for b in range(2)] for bit in thirds
    ]
    real = lane < nodes
    for o in range(OCT):
        plane = [xs[o // 4][i // 2] * ys[o // 2 % 2][i % 2] for i in range(nodes // 8)]
        for r, third in enumerate(zs):
            block = [value * third[o % 2] for value in plane]
            wide = jnp.concatenate(
                [jnp.where(real, value, 0.0) for value in block] + [jnp.where(real, 0.0, value) for value in block], 0
            )
            high = wide.astype(BF16)
            low = (wide - high.astype(F32)).astype(BF16)
            place[pl.ds((r * OCT + o) * 2 * nodes, 2 * nodes), :] = jnp.concatenate([high, low], 1)


def push(weights, t, register):
    pltpu.matmul_push_rhs(weights(t), staging_register=register, mxu_index=t % 2)


def stage(sums, weights):
    for t in range(2):
        push(weights, t, 0)
        pltpu.matmul_acc_lhs(sums[t], jnp.zeros(sums[t].shape, BF16), load_staged_rhs=0)
    for t in range(2, 6):
        push(weights, t, t // 2 - 1)


def staged_product(sums, tiles, weights):
    for t, tile in enumerate(tiles):
        pltpu.matmul_acc_lhs(sums[t % 2], split_rows(tile), load_staged_rhs=(None, 0, 1, 0)[t // 2])
        if t // 2 == 1:
            push(weights, t + 4, 0)
    return collect(sums, tiles)


def product(sums, tiles, weights):
    for t, tile in enumerate(tiles):
        push(weights, t, t // 2 % 2)
        pltpu.matmul_acc_lhs(sums[t % 2], split_rows(tile), load_staged_rhs=t // 2 % 2)
    return collect(sums, tiles)


def collect(sums, tiles):
    rows, width = tiles[0].shape
    parts = [fold(pltpu.matmul_pop(total), rows, width // 2) for total in sums[: len(tiles)]]
    return functools.reduce(jnp.add, parts)


def kernel(halves, blks, subs, cones, sizes, *refs):
    specs = [pltpu.ACC(unit)((rows, 2 * refs[0].shape[-1]), F32) for rows in sizes for unit in range(2)]

    def inside(*totals):
        for total in totals:
            pltpu.matmul_pop(total)
        sums = {rows: totals[2 * i : 2 * i + 2] for i, rows in enumerate(sizes)}
        upward(halves, blks, subs, cones, sums, *refs)

    pl.run_scoped(inside, *specs)


def upward(
    halves, blks, subs, cones, sums,
    leaf_hbm, occ_hbm, angle_hbm, need3_hbm, need4_hbm,
    low_out, cone_out,
    leaf, occ, keep, angle, need3, need4, both, weight, part, got, mine, theirs, near, far, four,
    in_sem, send, recv, recv2, ready,
):
    groups = halves * blks
    half, blk, sub = lax.axis_index("half"), lax.axis_index("blk"), lax.axis_index("sub")
    group = half * blks + blk
    pairs, family, width = leaf_hbm.shape
    nodes = width // 2
    per_sub = pairs // subs

    pltpu.make_async_copy(occ_hbm, occ, in_sem.at[0]).start()
    for q in range(family):
        pltpu.make_async_copy(leaf_hbm.at[:, q], leaf.at[pl.ds(q * pairs, pairs)], in_sem.at[1]).start()
    loads = [
        pltpu.make_async_copy(src, dst, in_sem.at[2 + i])
        for i, (src, dst) in enumerate([(angle_hbm, angle), (need3_hbm, need3), (need4_hbm, need4)])
    ]
    for load in loads:
        load.start()

    other = halves - 1 - half

    def blk_of(j):
        return lax.rem(j + blks - 1 - blk, blks)

    def sub_of(t):
        return lax.rem(t + subs - 1 - sub, subs)

    def peer(d):
        return {"half": other, "blk": blk_of(d // subs), "sub": sub_of(lax.rem(d, subs))}

    def planes(wanted, act):
        def plane(j):
            @pl.when(wanted(blk_of(j), blk))
            def _():
                each(0, subs, lambda t: act(j * subs + t))

        each(0, blks, plane)

    level = lax.rem(2 * blk + 1, blks)

    def beside(wanted, act):
        def device(t):
            @pl.when(wanted(sub_of(t), sub))
            def _():
                act(level * subs + t)

        each(0, subs, device)

    def greet(semaphore):
        return lambda d: pl.semaphore_signal(semaphore, inc=1, device_id=peer(d), device_id_type=MESH)

    def across(t):
        return {"blk": blk_of(0), "sub": sub_of(t)}

    def greet_across(semaphore):
        each(0, subs, lambda t: pl.semaphore_signal(semaphore, inc=1, device_id=across(t), device_id_type=MESH))

    is_first, is_last = blk == 0, blk == blks - 1
    is_end = lax.rem(blk, blks - 1) == 0
    barrier = pltpu.get_barrier_semaphore()
    planes(operator.gt, greet(barrier))
    beside(operator.ge, greet(barrier))

    @pl.when(is_first)
    def _():
        greet_across(barrier)

    table = axis_table()
    then = np.einsum("bij,qjk->bqik", table, table)
    build(table, then, (lax.rem(sub // 2, 2), lax.rem(sub, 2), (0, 1)), nodes, both)

    pl.semaphore_wait(barrier, (blk + is_last.astype(jnp.int32)) * subs + sub + 1)

    @pl.when(is_last)
    def _():
        greet_across(ready.at[0])

    planes(operator.lt, lambda d: greet(ready.at[d // subs])(d))
    beside(operator.lt, greet(ready.at[level]))
    pltpu.make_async_copy(occ_hbm, occ, in_sem.at[0]).wait()
    lane = lax.broadcasted_iota(jnp.int32, (8, width), 1)
    own = lane // family == lax.broadcasted_iota(jnp.int32, (8, width), 0)
    flags = occ[...] << lax.rem(lane, family)[: occ.shape[0]]
    taken = [
        jnp.sum(jnp.where(own, jnp.broadcast_to(flags[i : i + 1].astype(F32), (8, width)), 0.0), 1, keepdims=True)
        for i in range(pairs // 8)
    ]
    taken = jnp.broadcast_to(jnp.concatenate(taken, 0).astype(jnp.int32), (pairs, width))
    for q in range(family):
        keep[q * pairs : (q + 1) * pairs, :] = jnp.where((taken & (1 << q)) != 0, 1.0, 0.0)

    def first_weights(t):
        return both[2 * width * t : 2 * width * (t + 1), :]

    stage(sums[2 * pairs], first_weights)
    pltpu.make_async_copy(leaf, leaf, in_sem.at[1]).wait()
    masked = [leaf[q * pairs : (q + 1) * pairs, :] * keep[q * pairs : (q + 1) * pairs, :] for q in range(family)]
    part[...] = staged_product(
        sums[2 * pairs], [jnp.concatenate(masked[2 * t : 2 * t + 2], 1) for t in range(family // 2)], first_weights
    )

    def copy(d, there=None):
        there = peer(d) if there is None else there
        j = d // subs
        return pltpu.make_async_remote_copy(
            src_ref=part.at[pl.ds(pl.multiple_of(there["sub"] * per_sub, 8), per_sub)],
            dst_ref=got.at[jnp.where(j == 0, half, j + 1) * subs + sub],
            send_sem=send.at[0],
            recv_sem=recv.at[jnp.minimum(j, 1)],
            device_id=there,
            device_id_type=MESH,
        )

    def copy_across(order):
        for to in order:
            each(0, subs, lambda t: copy(t, {"half": to, **across(t)}).start())

    @pl.when(is_last)
    def _():
        copy_across(range(halves))

    def inward(there):
        @pl.when(jnp.logical_and(there < blk, there + blks - 1 != blk))
        def _():
            j = lax.rem(blk + there + 1, blks)
            each(0, subs, lambda t: copy(j * subs + t).start())

    each(0, blks - 1, inward)
    beside(operator.le, lambda d: copy(d).start())

    build(table, then, (None, None, (None,)), nodes, weight)

    loads[0].wait()
    padded = near.shape[2]
    count = angle.shape[1]
    pick = lax.broadcasted_iota(jnp.int32, (padded, count), 1) == (
        lax.broadcasted_iota(jnp.int32, (padded, count), 0) + group * cones
    )
    polar = jnp.sum(jnp.where(pick, angle[0:1, :], 0.0), 1, keepdims=True)
    azimuth = jnp.sum(jnp.where(pick, angle[1:2, :], 0.0), 1, keepdims=True)
    sin_polar = jnp.sin(polar)
    direction = [sin_polar * jnp.cos(azimuth), sin_polar * jnp.sin(azimuth), jnp.cos(polar)]
    lane = lax.broadcasted_iota(jnp.int32, (padded, width), 1)
    points = [float(value) for value in chebyshev_points(ORDER)]
    places = [choose(digit_of(lane, ORDER**power), points) for power in (2, 1, 0)]
    sign = jnp.where(lane < nodes, -1.0, 1.0)
    for load in loads[1:]:
        load.wait()

    def widen(value):
        fill = padded - cones
        if fill:
            value = jnp.concatenate([value, jnp.zeros((fill, value.shape[1]), value.dtype)], 0)
        return value.astype(F32)

    keep3 = widen(need3[...])
    signs = octant_signs()
    for o in range(OCT):
        argument = sum(
            axis * (place + float(signs[o, d])) for d, (axis, place) in enumerate(zip(direction, places))
        ) * -NEAR
        cosine, sine = jnp.cos(argument), jnp.sin(argument)
        near[0, o] = cosine
        near[1, o] = sine * sign
        for g in range(o, groups, OCT):
            kept = keep3[:, g : g + 1]
            far[0, g] = (1.0 - 2.0 * sine * sine) * kept
            far[1, g] = 2.0 * sine * cosine * sign * kept
    lanes4 = need4.shape[1]
    diagonal = lax.broadcasted_iota(jnp.int32, (padded, lanes4), 0) == lax.broadcasted_iota(
        jnp.int32, (padded, lanes4), 1
    )
    keep4 = [
        jnp.sum(jnp.where(diagonal, need4[q : q + 1, :].astype(F32), 0.0), 1, keepdims=True)
        for q in range(groups // OCT)
    ]

    def outward(k):
        @pl.when(blk + k < blks)
        def _():
            if k == blks - 1:
                pl.semaphore_wait(ready.at[0], halves * subs)
                copy_across(reversed(range(halves)))
            else:
                j = lax.rem(2 * blk + k + 1, blks)
                pl.semaphore_wait(ready.at[j], subs)
                each(0, subs, lambda t: copy(j * subs + t).start())

    @pl.when(sub < subs - 1)
    def _():
        pl.semaphore_wait(ready.at[level], subs - 1 - sub)
        beside(operator.gt, lambda d: copy(d).start())

    each(1, blks, outward)

    def rows_of(base, start, size):
        return weight[pl.ds(pl.multiple_of(base + start, nodes), size), :]

    def turning(o):
        base = lax.rem(o, OCT) * width
        return jnp.concatenate([rows_of(base, 0, width), rows_of(base, nodes, nodes), rows_of(base, 0, nodes)], 0)

    def level_three(places, multiply):
        boxes = [(mine, theirs)[own][j] for own, j in places]
        tiles = [
            jnp.concatenate(
                [
                    jnp.concatenate([near[0, o] * box[o : o + 1, :], near[1, o] * -box[o : o + 1, :]], 1)
                    for box in boxes
                ],
                0,
            )
            for o in range(OCT)
        ]
        result = multiply(sums[2 * padded * len(places)], tiles, turning)
        index = [(other, half)[own] * blks + blk_of(j) for own, j in places]
        return [(g, result[i * padded : (i + 1) * padded]) for i, g in enumerate(index)]

    def level_four(found):
        tiles = [jnp.concatenate([far[0, g] * box, far[1, g] * -box], 1) for g, box in found]
        return product(sums[2 * padded], tiles, lambda t: turning(found[t][0]))

    last, rest = pl.ds(0, 1), pl.ds(1, blks - 1)

    def landed(semaphore, first, count):
        slots = got.at[pl.ds(first * subs, count * subs)]
        pltpu.make_async_copy(slots, slots, semaphore).wait()

    def total(slot):
        return functools.reduce(jnp.add, [got[slot * subs + t] for t in range(subs)])

    def forward(k):
        boxes = last if k == 0 else rest
        return pltpu.make_async_remote_copy(
            src_ref=mine.at[boxes],
            dst_ref=theirs.at[boxes],
            send_sem=send.at[0],
            recv_sem=recv2.at[0],
            device_id={"half": other},
            device_id_type=MESH,
        )

    landed(recv.at[1], halves, blks - 1)
    for j in range(1, blks):
        mine[j] = total(j + 1)
    forward(1).start()

    @pl.when(jnp.logical_not(is_end))
    def _():
        landed(recv.at[0], other, 1)
        mine[0] = total(other)
        forward(0).start()

    single = groups == OCT
    direct = [(0, j) for j in range(1, blks)]
    handed = [(1, j) for j in range(1, blks)] + [(0, 0), (1, 0)]
    if single:
        early = level_four(level_three(direct, product))
        stage(sums[2 * padded * len(handed)], turning)

    def handed_over(boxes):
        pltpu.make_async_copy(theirs.at[boxes], theirs.at[boxes], recv2.at[0]).wait()

    @pl.when(is_end)
    def _():
        handed_over(rest)
        landed(recv.at[0], 0, halves)
        mine[0] = total(other)
        theirs[0] = total(half)

    @pl.when(jnp.logical_not(is_end))
    def _():
        handed_over(pl.ds(0, blks))

    if single:
        cone_out[:, 0, :] = ((early + level_four(level_three(handed, staged_product))) * keep4[0])[:cones]
    else:
        four[...] = jnp.zeros_like(four)
        together = direct + handed
        for start in range(0, len(together), 6):
            for g, box in level_three(together[start : start + 6], product):
                four[g // OCT] += level_four([(g, box)])
        for q in range(groups // OCT):
            cone_out[:, q, :] = (four[q] * keep4[q])[:cones]
    low_out[...] = theirs[level]

    def sent(count):
        slots = got.at[pl.ds(0, count)]
        pltpu.make_async_copy(slots, slots, send.at[0]).wait()

    @pl.when(is_end)
    def _():
        sent((blks + 1) * subs + blks - 1)

    @pl.when(jnp.logical_not(is_end))
    def _():
        sent(blks * subs + blks)


def put_out(low_ref, cone_ref, low_out, cone_out, sems):
    copies = [
        pltpu.make_async_copy(low_ref, low_out, sems.at[0]),
        pltpu.make_async_copy(cone_ref, cone_out, sems.at[1]),
    ]
    for copy in copies:
        copy.start()
    for copy in copies:
        copy.wait()


def solution(mesh):
    halves, blks, subs = mesh.shape["half"], mesh.shape["blk"], mesh.shape["sub"]
    groups = halves * blks

    def local(leaf, occupied, angles, need3, need4):
        rows, width = leaf.shape
        family = 2 * OCT
        pairs = rows // family
        per_sub = pairs // subs
        cones = need3.shape[0]
        padded = -(-cones // 8) * 8
        assert per_sub == OCT and need3.shape[1] == groups and halves == 2 and subs * 2 == OCT
        assert width == 2 * ORDER**3 and blks % 2 == 0
        boxes = (blks - 1, blks + 1) if groups == OCT else (6, 2 * blks % 6)
        sizes = sorted({2 * pairs, 2 * padded} | {2 * padded * count for count in boxes if count})
        leaf = leaf.reshape(pairs, family, width)
        occupied = occupied.reshape(rows // 128, 128)
        need4 = need4.T
        vmem = pl.BlockSpec(memory_space=pltpu.VMEM)
        anywhere = pl.BlockSpec(memory_space=pl.ANY)
        results = pl.pallas_call(
            functools.partial(kernel, halves, blks, subs, cones, sizes),
            out_shape=(
                pltpu.VMEM((per_sub, width), F32),
                pltpu.VMEM((cones, groups // OCT, width), F32),
            ),
            in_specs=[anywhere] * 5,
            out_specs=(vmem, vmem),
            scratch_shapes=[
                pltpu.VMEM((rows, width), F32),
                pltpu.VMEM(occupied.shape, jnp.int32),
                pltpu.VMEM((rows, width), F32),
                pltpu.VMEM(angles.shape, F32),
                pltpu.VMEM(need3.shape, jnp.int32),
                pltpu.VMEM(need4.shape, jnp.int32),
                pltpu.VMEM((family * width, 2 * width), BF16),
                pltpu.VMEM((OCT * width, 2 * width), BF16),
                pltpu.VMEM((pairs, width), F32),
                pltpu.VMEM(((blks + 1) * subs + blks, per_sub, width), F32),
                pltpu.VMEM((blks, per_sub, width), F32),
                pltpu.VMEM((blks, per_sub, width), F32),
                pltpu.VMEM((2, OCT, padded, width), F32),
                pltpu.VMEM((2, groups, padded, width), F32),
                pltpu.VMEM((groups // OCT, padded, width), F32),
                pltpu.SemaphoreType.DMA((5,)),
                pltpu.SemaphoreType.DMA((1,)),
                pltpu.SemaphoreType.DMA((2,)),
                pltpu.SemaphoreType.DMA((1,)),
                pltpu.SemaphoreType.REGULAR((blks,)),
            ],
            compiler_params=pltpu.CompilerParams(collective_id=0, has_side_effects=True),
            name="upward",
        )(leaf, occupied, angles, need3, need4)
        results = [pltpu.with_memory_space_constraint(value, pltpu.VMEM) for value in results]
        return pl.pallas_call(
            put_out,
            out_shape=[jax.ShapeDtypeStruct(value.shape, F32) for value in results],
            in_specs=[vmem] * 2,
            out_specs=[pl.BlockSpec(memory_space=pltpu.HBM)] * 2,
            scratch_shapes=[pltpu.SemaphoreType.DMA((2,))],
            name="put_out",
        )(*results)

    return jax.shard_map(
        local,
        mesh=mesh,
        in_specs=(
            P(("half", "blk", "sub"), None),
            P(("half", "blk", "sub")),
            P(),
            P(("half", "blk"), "sub"),
            P(("half", "blk"), "sub"),
        ),
        out_specs=(P(("half", "blk", "sub"), None), P(("half", "blk"), "sub", None)),
        check_vma=False,
    )
```

```python
import functools
import math
import operator

import jax
import jax.numpy as jnp
import numpy as np
from jax import lax
from jax.experimental import pallas as pl
from jax.experimental.pallas import tpu as pltpu
from jax.sharding import PartitionSpec as P

MESH = pl.DeviceIdType.MESH
F32, BF16 = jnp.float32, jnp.bfloat16
ORDER = 4
OCT = 8
NEAR = 1.5


def octant_signs():
    octant = np.arange(OCT)
    return np.stack([octant // 4 % 2, octant // 2 % 2, octant % 2], -1) * 2.0 - 1.0


def chebyshev_points(per_axis):
    return np.cos((2.0 * np.arange(per_axis) + 1.0) * math.pi / (2.0 * per_axis))


def axis_table():
    points = chebyshev_points(ORDER)
    degree = np.arange(1, ORDER)
    shifted = (points[None, :] + np.array([-1.0, 1.0])[:, None]) / 2.0
    here = np.cos(degree[None, :] * np.arccos(points)[:, None])
    there = np.cos(degree * np.arccos(shifted)[:, :, None])
    return 1.0 / ORDER + 2.0 / ORDER * np.einsum("mk,bnk->bnm", here, there)


def each(start, count, body):
    if count - start <= 64:
        for d in range(start, count):
            body(d)
    else:
        lax.fori_loop(start, count, lambda d, c: (body(d), c)[1], 0)


def split_rows(value):
    high = value.astype(BF16).astype(F32)
    return jnp.concatenate([high, value - high], 0).astype(BF16)


def fold(acc, rows, width):
    return (acc[:rows, :width] + acc[rows:, :width]) + (acc[:rows, width:] + acc[rows:, width:])


def choose(digit, values):
    return jnp.where(
        digit < 2, jnp.where(digit == 0, values[0], values[1]), jnp.where(digit == 2, values[2], values[3])
    )


def digit_of(index, place):
    return lax.rem(index // place, ORDER)


def build(table, then, bits, nodes, place):
    tile = (8, 2 * nodes)
    row, lane = lax.broadcasted_iota(jnp.int32, tile, 0), lax.broadcasted_iota(jnp.int32, tile, 1)

    def along(first, bit, i, stride):
        if bit is None:
            values = [float(table[first, i, j]) for j in range(ORDER)]
        elif isinstance(bit, int):
            values = [float(then[first, bit, i, j]) for j in range(ORDER)]
        else:
            values = [
                jnp.where(bit == 0, float(then[first, 0, i, j]), float(then[first, 1, i, j]))
                for j in range(ORDER)
            ]
        return choose(digit_of(lane, stride), values)

    bit_x, bit_y, thirds = bits
    xs = [[along(b, bit_x, i, ORDER * ORDER) for i in range(ORDER)] for b in range(2)]
    ys = [
        [jnp.where(row < ORDER, along(b, bit_y, 2 * i, ORDER), along(b, bit_y, 2 * i + 1, ORDER)) for i in range(2)]
        for b in range(2)
    ]
    zs = [
        [choose(digit_of(row, 1), [along(b, bit, i, 1) for i in range(ORDER)]) for b in range(2)] for bit in thirds
    ]
    real = lane < nodes
    for o in range(OCT):
        plane = [xs[o // 4][i // 2] * ys[o // 2 % 2][i % 2] for i in range(nodes // 8)]
        for r, third in enumerate(zs):
            block = [value * third[o % 2] for value in plane]
            wide = jnp.concatenate(
                [jnp.where(real, value, 0.0) for value in block] + [jnp.where(real, 0.0, value) for value in block], 0
            )
            high = wide.astype(BF16)
            low = (wide - high.astype(F32)).astype(BF16)
            place[pl.ds((r * OCT + o) * 2 * nodes, 2 * nodes), :] = jnp.concatenate([high, low], 1)


def push(weights, t, register):
    pltpu.matmul_push_rhs(weights(t), staging_register=register, mxu_index=t % 2)


def stage(sums, weights):
    for t in range(2):
        push(weights, t, 0)
        pltpu.matmul_acc_lhs(sums[t], jnp.zeros(sums[t].shape, BF16), load_staged_rhs=0)
    for t in range(2, 6):
        push(weights, t, t // 2 - 1)


def staged_product(sums, tiles, weights):
    for t, tile in enumerate(tiles):
        pltpu.matmul_acc_lhs(sums[t % 2], split_rows(tile), load_staged_rhs=(None, 0, 1, 0)[t // 2])
        if t // 2 == 1:
            push(weights, t + 4, 0)
    return collect(sums, tiles)


def product(sums, tiles, weights):
    for t, tile in enumerate(tiles):
        push(weights, t, t // 2 % 2)
        pltpu.matmul_acc_lhs(sums[t % 2], split_rows(tile), load_staged_rhs=t // 2 % 2)
    return collect(sums, tiles)


def collect(sums, tiles):
    rows, width = tiles[0].shape
    parts = [fold(pltpu.matmul_pop(total), rows, width // 2) for total in sums[: len(tiles)]]
    return functools.reduce(jnp.add, parts)


def kernel(halves, blks, subs, cones, sizes, *refs):
    specs = [pltpu.ACC(unit)((rows, 2 * refs[0].shape[-1]), F32) for rows in sizes for unit in range(2)]

    def inside(*totals):
        for total in totals:
            pltpu.matmul_pop(total)
        sums = {rows: totals[2 * i : 2 * i + 2] for i, rows in enumerate(sizes)}
        upward(halves, blks, subs, cones, sums, *refs)

    pl.run_scoped(inside, *specs)


def upward(
    halves, blks, subs, cones, sums,
    leaf_hbm, occ_hbm, angle_hbm, need3_hbm, need4_hbm,
    low_out, cone_out,
    leaf, occ, keep, angle, need3, need4, both, weight, part, got, mine, theirs, near, far, four,
    in_sem, recv, recv2, ready,
):
    groups = halves * blks
    half, blk, sub = lax.axis_index("half"), lax.axis_index("blk"), lax.axis_index("sub")
    group = half * blks + blk
    pairs, family, width = leaf_hbm.shape
    nodes = width // 2
    per_sub = pairs // subs

    pltpu.make_async_copy(occ_hbm, occ, in_sem.at[0]).start()
    for q in range(family):
        pltpu.make_async_copy(leaf_hbm.at[:, q], leaf.at[pl.ds(q * pairs, pairs)], in_sem.at[1]).start()
    loads = [
        pltpu.make_async_copy(src, dst, in_sem.at[0])
        for src, dst in [(angle_hbm, angle), (need3_hbm, need3), (need4_hbm, need4)]
    ]

    other = halves - 1 - half

    def blk_of(j):
        return lax.rem(j + blks - 1 - blk, blks)

    def sub_of(t):
        return lax.rem(t + subs - 1 - sub, subs)

    def peer(d):
        return {"half": other, "blk": blk_of(d // subs), "sub": sub_of(lax.rem(d, subs))}

    def planes(wanted, act):
        def plane(j):
            @pl.when(wanted(blk_of(j), blk))
            def _():
                each(0, subs, lambda t: act(j * subs + t))

        each(0, blks, plane)

    level = lax.rem(2 * blk + 1, blks)

    def beside(wanted, act):
        def device(t):
            @pl.when(wanted(sub_of(t), sub))
            def _():
                act(level * subs + t)

        each(0, subs, device)

    def greet(semaphore):
        return lambda d: pl.semaphore_signal(semaphore, inc=1, device_id=peer(d), device_id_type=MESH)

    def across(t):
        return {"blk": blk_of(0), "sub": sub_of(t)}

    def greet_across(semaphore):
        each(0, subs, lambda t: pl.semaphore_signal(semaphore, inc=1, device_id=across(t), device_id_type=MESH))

    is_first, is_last = blk == 0, blk == blks - 1
    is_end = lax.rem(blk, blks - 1) == 0
    barrier = pltpu.get_barrier_semaphore()
    planes(operator.gt, greet(barrier))
    beside(operator.ge, greet(barrier))

    @pl.when(is_first)
    def _():
        greet_across(barrier)

    table = axis_table()
    then = np.einsum("bij,qjk->bqik", table, table)
    build(table, then, (lax.rem(sub // 2, 2), lax.rem(sub, 2), (0, 1)), nodes, both)

    pl.semaphore_wait(barrier, (blk + is_last.astype(jnp.int32)) * subs + sub + 1)

    @pl.when(is_last)
    def _():
        greet_across(ready.at[0])

    planes(operator.lt, lambda d: greet(ready.at[d // subs])(d))
    beside(operator.lt, greet(ready.at[level]))
    pltpu.make_async_copy(occ_hbm, occ, in_sem.at[0]).wait()
    loads[0].start()
    lane = lax.broadcasted_iota(jnp.int32, (8, width), 1)
    own = lane // family == lax.broadcasted_iota(jnp.int32, (8, width), 0)
    flags = occ[...] << lax.rem(lane, family)[: occ.shape[0]]
    taken = [
        jnp.sum(jnp.where(own, jnp.broadcast_to(flags[i : i + 1].astype(F32), (8, width)), 0.0), 1, keepdims=True)
        for i in range(pairs // 8)
    ]
    taken = jnp.broadcast_to(jnp.concatenate(taken, 0).astype(jnp.int32), (pairs, width))
    for q in range(family):
        keep[q * pairs : (q + 1) * pairs, :] = jnp.where((taken & (1 << q)) != 0, 1.0, 0.0)

    def first_weights(t):
        return both[2 * width * t : 2 * width * (t + 1), :]

    stage(sums[2 * pairs], first_weights)
    pltpu.make_async_copy(leaf, leaf, in_sem.at[1]).wait()
    masked = [leaf[q * pairs : (q + 1) * pairs, :] * keep[q * pairs : (q + 1) * pairs, :] for q in range(family)]
    part[...] = staged_product(
        sums[2 * pairs], [jnp.concatenate(masked[2 * t : 2 * t + 2], 1) for t in range(family // 2)], first_weights
    )

    def copy(d, there=None):
        there = peer(d) if there is None else there
        j = d // subs
        return pltpu.make_async_remote_copy(
            src_ref=part.at[pl.ds(pl.multiple_of(there["sub"] * per_sub, 8), per_sub)],
            dst_ref=got.at[jnp.where(j == 0, half, j + 1) * subs + sub],
            send_sem=in_sem.at[1],
            recv_sem=recv.at[jnp.minimum(j, 1)],
            device_id=there,
            device_id_type=MESH,
        )

    def copy_across(to, t):
        copy(t, {"half": to, **across(t)}).start()

    @pl.when(is_last)
    def _():
        for to in range(halves):
            each(0, subs, lambda t: copy_across(to, t))

    def inward(there):
        @pl.when(jnp.logical_and(there < blk, there + blks - 1 != blk))
        def _():
            j = lax.rem(blk + there + 1, blks)
            each(0, subs, lambda t: copy(j * subs + t).start())

    each(0, blks - 1, inward)
    beside(operator.le, lambda d: copy(d).start())

    loads[0].wait()
    loads[1].start()
    build(table, then, (None, None, (None,)), nodes, weight)
    padded = near.shape[2]
    count = angle.shape[1]
    pick = lax.broadcasted_iota(jnp.int32, (padded, count), 1) == (
        lax.broadcasted_iota(jnp.int32, (padded, count), 0) + group * cones
    )
    polar = jnp.sum(jnp.where(pick, angle[0:1, :], 0.0), 1, keepdims=True)
    azimuth = jnp.sum(jnp.where(pick, angle[1:2, :], 0.0), 1, keepdims=True)
    sin_polar = jnp.sin(polar)
    direction = [sin_polar * jnp.cos(azimuth), sin_polar * jnp.sin(azimuth), jnp.cos(polar)]
    lane = lax.broadcasted_iota(jnp.int32, (padded, width), 1)
    points = [float(value) for value in chebyshev_points(ORDER)]
    places = [choose(digit_of(lane, ORDER**power), points) for power in (2, 1, 0)]
    sign = jnp.where(lane < nodes, -1.0, 1.0)
    loads[1].wait()
    loads[2].start()

    def widen(value):
        fill = padded - cones
        if fill:
            value = jnp.concatenate([value, jnp.zeros((fill, value.shape[1]), value.dtype)], 0)
        return value.astype(F32)

    keep3 = widen(need3[...])
    signs = octant_signs()
    for o in range(OCT):
        argument = sum(
            axis * (place + float(signs[o, d])) for d, (axis, place) in enumerate(zip(direction, places))
        ) * -NEAR
        cosine, sine = jnp.cos(argument), jnp.sin(argument)
        near[0, o] = cosine
        near[1, o] = sine * sign
        for g in range(o, groups, OCT):
            kept = keep3[:, g : g + 1]
            far[0, g] = (1.0 - 2.0 * sine * sine) * kept
            far[1, g] = 2.0 * sine * cosine * sign * kept
    def outward(k):
        @pl.when(blk + k < blks)
        def _():
            if k == blks - 1:
                pl.semaphore_wait(ready.at[0], halves * subs)
                each(0, subs, lambda t: [copy_across(to, t) for to in reversed(range(halves))])
            else:
                j = lax.rem(2 * blk + k + 1, blks)
                pl.semaphore_wait(ready.at[j], subs)
                each(0, subs, lambda t: copy(j * subs + t).start())

    @pl.when(sub < subs - 1)
    def _():
        pl.semaphore_wait(ready.at[level], subs - 1 - sub)
        beside(operator.gt, lambda d: copy(d).start())

    each(1, blks, outward)

    def rows_of(base, start, size):
        return weight[pl.ds(pl.multiple_of(base + start, nodes), size), :]

    def turning(o):
        base = lax.rem(o, OCT) * width
        return jnp.concatenate([rows_of(base, 0, width), rows_of(base, nodes, nodes), rows_of(base, 0, nodes)], 0)

    def level_three(places, multiply):
        boxes = [(mine, theirs)[own][j] for own, j in places]
        tiles = [
            jnp.concatenate(
                [
                    jnp.concatenate([near[0, o] * box[o : o + 1, :], near[1, o] * -box[o : o + 1, :]], 1)
                    for box in boxes
                ],
                0,
            )
            for o in range(OCT)
        ]
        result = multiply(sums[2 * padded * len(places)], tiles, turning)
        index = [(other, half)[own] * blks + blk_of(j) for own, j in places]
        return [(g, result[i * padded : (i + 1) * padded]) for i, g in enumerate(index)]

    def level_four(found):
        tiles = [jnp.concatenate([far[0, g] * box, far[1, g] * -box], 1) for g, box in found]
        return product(sums[2 * padded], tiles, lambda t: turning(found[t][0]))

    last, rest = pl.ds(0, 1), pl.ds(1, blks - 1)

    def landed(semaphore, first, count):
        slots = got.at[pl.ds(first * subs, count * subs)]
        pltpu.make_async_copy(slots, slots, semaphore).wait()

    def total(slot):
        return functools.reduce(jnp.add, [got[slot * subs + t] for t in range(subs)])

    def forward(k):
        boxes = last if k == 0 else rest
        return pltpu.make_async_remote_copy(
            src_ref=mine.at[boxes],
            dst_ref=theirs.at[boxes],
            send_sem=in_sem.at[1],
            recv_sem=recv2.at[0],
            device_id={"half": other},
            device_id_type=MESH,
        )

    landed(recv.at[1], halves, blks - 1)
    for j in range(1, blks):
        mine[j] = total(j + 1)
    forward(1).start()

    @pl.when(jnp.logical_not(is_end))
    def _():
        landed(recv.at[0], other, 1)
        mine[0] = total(other)
        forward(0).start()

    loads[2].wait()
    lanes4 = need4.shape[1]
    diagonal = lax.broadcasted_iota(jnp.int32, (padded, lanes4), 0) == lax.broadcasted_iota(
        jnp.int32, (padded, lanes4), 1
    )
    keep4 = [
        jnp.sum(jnp.where(diagonal, need4[q : q + 1, :].astype(F32), 0.0), 1, keepdims=True)
        for q in range(groups // OCT)
    ]

    single = groups == OCT
    direct = [(0, j) for j in range(1, blks)]
    handed = [(1, j) for j in range(1, blks)] + [(0, 0), (1, 0)]
    if single:
        early = level_four(level_three(direct, product))
        stage(sums[2 * padded * len(handed)], turning)

    def handed_over(boxes):
        pltpu.make_async_copy(theirs.at[boxes], theirs.at[boxes], recv2.at[0]).wait()

    @pl.when(is_end)
    def _():
        handed_over(rest)
        landed(recv.at[0], 0, halves)
        mine[0] = total(other)
        theirs[0] = total(half)

    @pl.when(jnp.logical_not(is_end))
    def _():
        handed_over(pl.ds(0, blks))

    if single:
        cone_out[:, 0, :] = ((early + level_four(level_three(handed, staged_product))) * keep4[0])[:cones]
    else:
        four[...] = jnp.zeros_like(four)
        together = direct + handed
        for start in range(0, len(together), 6):
            for g, box in level_three(together[start : start + 6], product):
                four[g // OCT] += level_four([(g, box)])
        for q in range(groups // OCT):
            cone_out[:, q, :] = (four[q] * keep4[q])[:cones]
    low_out[...] = theirs[level]

    def sent(count):
        slots = got.at[pl.ds(0, count)]
        pltpu.make_async_copy(slots, slots, in_sem.at[1]).wait()

    @pl.when(is_end)
    def _():
        sent((blks + 1) * subs + blks - 1)

    @pl.when(jnp.logical_not(is_end))
    def _():
        sent(blks * subs + blks)


def put_out(low_ref, cone_ref, low_out, cone_out, sems):
    copies = [
        pltpu.make_async_copy(low_ref, low_out, sems.at[0]),
        pltpu.make_async_copy(cone_ref, cone_out, sems.at[1]),
    ]
    for copy in copies:
        copy.start()
    for copy in copies:
        copy.wait()


def solution(mesh):
    halves, blks, subs = mesh.shape["half"], mesh.shape["blk"], mesh.shape["sub"]
    groups = halves * blks

    def local(leaf, occupied, angles, need3, need4):
        rows, width = leaf.shape
        family = 2 * OCT
        pairs = rows // family
        per_sub = pairs // subs
        cones = need3.shape[0]
        padded = -(-cones // 8) * 8
        assert per_sub == OCT and need3.shape[1] == groups and halves == 2 and subs * 2 == OCT
        assert width == 2 * ORDER**3 and blks % 2 == 0
        boxes = (blks - 1, blks + 1) if groups == OCT else (6, 2 * blks % 6)
        sizes = sorted({2 * pairs, 2 * padded} | {2 * padded * count for count in boxes if count})
        leaf = leaf.reshape(pairs, family, width)
        occupied = occupied.reshape(rows // 128, 128)
        need4 = need4.T
        vmem = pl.BlockSpec(memory_space=pltpu.VMEM)
        anywhere = pl.BlockSpec(memory_space=pl.ANY)
        results = pl.pallas_call(
            functools.partial(kernel, halves, blks, subs, cones, sizes),
            out_shape=(
                pltpu.VMEM((per_sub, width), F32),
                pltpu.VMEM((cones, groups // OCT, width), F32),
            ),
            in_specs=[anywhere] * 5,
            out_specs=(vmem, vmem),
            scratch_shapes=[
                pltpu.VMEM((rows, width), F32),
                pltpu.VMEM(occupied.shape, jnp.int32),
                pltpu.VMEM((rows, width), F32),
                pltpu.VMEM(angles.shape, F32),
                pltpu.VMEM(need3.shape, jnp.int32),
                pltpu.VMEM(need4.shape, jnp.int32),
                pltpu.VMEM((family * width, 2 * width), BF16),
                pltpu.VMEM((OCT * width, 2 * width), BF16),
                pltpu.VMEM((pairs, width), F32),
                pltpu.VMEM(((blks + 1) * subs + blks, per_sub, width), F32),
                pltpu.VMEM((blks, per_sub, width), F32),
                pltpu.VMEM((blks, per_sub, width), F32),
                pltpu.VMEM((2, OCT, padded, width), F32),
                pltpu.VMEM((2, groups, padded, width), F32),
                pltpu.VMEM((groups // OCT, padded, width), F32),
                pltpu.SemaphoreType.DMA((2,)),
                pltpu.SemaphoreType.DMA((2,)),
                pltpu.SemaphoreType.DMA((1,)),
                pltpu.SemaphoreType.REGULAR((blks,)),
            ],
            compiler_params=pltpu.CompilerParams(collective_id=0, has_side_effects=True),
            name="upward",
        )(leaf, occupied, angles, need3, need4)
        results = [pltpu.with_memory_space_constraint(value, pltpu.VMEM) for value in results]
        return pl.pallas_call(
            put_out,
            out_shape=[jax.ShapeDtypeStruct(value.shape, F32) for value in results],
            in_specs=[vmem] * 2,
            out_specs=[pl.BlockSpec(memory_space=pltpu.HBM)] * 2,
            scratch_shapes=[pltpu.SemaphoreType.DMA((2,))],
            name="put_out",
        )(*results)

    return jax.shard_map(
        local,
        mesh=mesh,
        in_specs=(
            P(("half", "blk", "sub"), None),
            P(("half", "blk", "sub")),
            P(),
            P(("half", "blk"), "sub"),
            P(("half", "blk"), "sub"),
        ),
        out_specs=(P(("half", "blk", "sub"), None), P(("half", "blk"), "sub", None)),
        check_vma=False,
    )
```
